32 devices in a mesh: grp: 2 (over core), dp: 4 (over z), mp: 4 (over y, x).
Axes of the slice: x: 2, y: 2, z: 4, core: 2. Of those that a mesh axis runs over, the one named last changes fastest.
Arguments:
- hidden: bfloat16 [1024, 5120], P(('dp', 'mp')), may hold values from -6 to 6
- enc_weight: bfloat16 [5120, 8192], P(None, 'mp'), may hold values from -0.078125 to 0.078125
- enc_bias: bfloat16 [8192], P('mp'), may hold values from -5 to 5
- enc_frozen: bfloat16 [5120, 64], replicated, may hold values from -0.078125 to 0.078125
- enc_adapter: bfloat16 [64, 8192], P(None, 'mp'), may hold values from -0.75 to 0.75
- text_rows: bfloat16 [2560, 8192], P(('dp', 'mp')), may hold values from -6 to 6
- norm_gain: bfloat16 [8192], replicated, may hold values from 0.5 to 1.5
- value_weight: bfloat16 [8192, 1024], P(('dp', 'mp')), may hold values from -0.0625 to 0.0625
- value_bias: bfloat16 [1024], replicated, may hold values from -5 to 5
- llm_frozen: bfloat16 [8192, 64], P(('dp', 'mp')), may hold values from -0.0625 to 0.0625
- llm_adapter: bfloat16 [64, 1024], replicated, may hold values from -0.75 to 0.75
- targets: bfloat16 [2560, 1024], P(('dp', 'mp')), may hold values from -6 to 6
- dest_owner: int32 [1024, 1], replicated, may hold values from 0 to 15; in each aligned block of 256 rows (0 to 255, 256 to 511, ...) at most 32 rows name the same one
- seq_length: int32 [16], P(('dp', 'mp')), may hold values from 128 to 160
Outputs:
- grad_enc: float32 [64, 8192], P('grp', 'mp')
- grad_llm: float32 [64, 1024], P('grp')
The draws below stay inside these ranges and needn't reach their ends.
Inputs may be any that keep to these rules, and one draw needn't show every extreme that they name: `dest_owner`: within the tokens of one encoder block (aligned blocks of 256 rows) no LLM device is named more than 32 times, and some device is named exactly 32 times in some blocks.
All inputs are finite; a program needn't handle non-finite values.
Results may differ from the reference program's by a relative error of at most 0.003.
Values may be sent and summed in bfloat16 or wider, within the bound.
A program may use at most 128 MiB of HBM per device.

```python
import math
import jax
import jax.numpy as jnp
import numpy as np
from jax import lax

D = 8192
MH = 5120
KV = 1024
RANK = 64
ENC_DEV = 256
LLM_DEV = 160
OWNERS = 16
CAP = 32
IMG = 1024
N_DP = 4
N_MP = 4


def touch_ends(values, rng, low, top_value):
    shape = values.shape
    place = [jax.random.randint(jax.random.fold_in(rng, axis), (), 0, shape[axis]) for axis in range(len(shape))]
    values = values.at[tuple(place)].set(low)
    longest = shape.index(max(shape))
    place[longest] = (place[longest] + 1) % shape[longest]
    return values.at[tuple(place)].set(top_value)


def level_of(stream_key, dims, shards, low, top_value):
    def one(dim, parts):
        heights = jax.random.uniform(jax.random.fold_in(jax.random.fold_in(stream_key, 6), dim), (parts,), jnp.float32, low / len(shards), top_value / len(shards))
        return jnp.repeat(jnp.exp(heights), dims[dim] // parts).reshape((-1,) + (1,) * (len(dims) - dim - 1))

    factor_of = one(*shards[0])
    for cut in shards[1:]:
        factor_of = factor_of * one(*cut)
    return factor_of


def deal_out(key, own, number, rows, count, top, reach, slope):
    sequence = jax.random.permutation(key, count)
    heavy_load, common = shares(count, rows * top, reach, slope, True), shares(count, rows * top, reach, slope, False)
    places = jnp.arange(count)

    def named(sizes, offset_by):
        used = int((sizes > 0).sum())
        fixed = max(1, used // 4)
        moved = fixed + (places - fixed + offset_by * (used - fixed)) % max(1, count - fixed)
        return jnp.zeros((count,), jnp.int32).at[sequence[jnp.where(places < fixed, places, moved)]].set(jnp.asarray(sizes, jnp.int32))

    sizes = jnp.where(number % 4 == 0, named(heavy_load, number // 4), named(common, number - number // 4 - 1))
    mixed = jax.random.permutation(jax.random.fold_in(own, 3), count)
    donor, sink = mixed[0:count // 2 * 2:2], mixed[1:count // 2 * 2:2]
    room = jnp.minimum(sizes[donor] - 1, reach - sizes[sink]) // 2
    room = jnp.where((donor == sequence[0]) | (sink == sequence[0]) | (sizes[sink] == 0), 0, jnp.maximum(room, 0))
    moved = jax.random.randint(jax.random.fold_in(own, 4), (count // 2,), 0, 1 << 20) % (room + 1)
    sizes = sizes.at[donor].add(-moved).at[sink].add(moved)
    items = jnp.searchsorted(jnp.cumsum(sizes), jnp.arange(rows * top), side="right").astype(jnp.int32)
    listing = items.reshape(top, rows).T
    listing = listing[jax.random.permutation(jax.random.fold_in(own, 1), rows)]
    offset_by = jax.random.randint(jax.random.fold_in(own, 2), (rows, 1), 0, top)
    return jnp.take_along_axis(listing, (jnp.arange(top)[None, :] + offset_by) % top, axis=1)


def shares(number_of, total, most, slope, full):
    portions = [(1 << 20) // math.isqrt(grade ** slope) + 1 for grade in range(1, number_of + 1)]
    largest = most if full else min(most, max(-(-total // number_of), total * portions[0] // sum(portions)))
    least = 1 if total - largest >= number_of - 1 else 0
    given, surplus = [largest] + [least] * (number_of - 1), total - largest - least * (number_of - 1)
    while surplus > 0:
        candidates = [i for i in range(1, number_of) if given[i] < largest] or [i for i in range(1, number_of) if given[i] < most]
        pool, left = sum([portions[i] for i in candidates]), surplus
        for i in candidates:
            extra = min(most - given[i], max(1, left * portions[i] // pool), surplus)
            given[i] = given[i] + extra
            surplus = surplus - extra
    return np.array(given)


def noise(own_key, dims, scale, most, shards=(), kind=jnp.bfloat16):
    values = scale * jax.random.normal(own_key, dims, jnp.float32)
    if shards:
        values = values * level_of(own_key, dims, shards, -0.22, 0.18)
    return jnp.clip(values, -most, most).astype(kind)


def setup_inputs(seed: int = 0) -> dict:
    streams_of = jax.random.split(jax.random.key(seed), 15)
    hidden = noise(streams_of[0], (IMG, MH), 1.0, 6.0, ((0, 16),))
    enc_weight = noise(streams_of[1], (MH, D), MH ** -0.5, 0.078125, ((1, 4),))
    enc_bias = noise(streams_of[2], (D,), 1.0, 5.0, ((0, 4),))
    enc_frozen = noise(streams_of[3], (MH, RANK), MH ** -0.5, 0.078125)
    enc_adapter = noise(streams_of[4], (RANK, D), RANK ** -0.5, 0.75, ((1, 4),))
    text_rows = noise(streams_of[5], (OWNERS * LLM_DEV, D), 1.0, 6.0, ((0, 16),))
    norm_gain = jnp.clip(1.0 + 0.1 * jax.random.normal(streams_of[6], (D,), jnp.float32), 0.5, 1.5).astype(jnp.bfloat16)
    value_weight = noise(streams_of[7], (D, KV), D ** -0.5, 0.0625, ((0, 16),))
    value_bias = noise(streams_of[8], (KV,), 1.0, 5.0)
    llm_frozen = noise(streams_of[9], (D, RANK), D ** -0.5, 0.0625, ((0, 16),))
    llm_adapter = noise(streams_of[10], (RANK, KV), RANK ** -0.5, 0.75)
    targets = noise(streams_of[11], (OWNERS * LLM_DEV, KV), 1.0, 6.0, ((0, 16),))
    dest_owner_keys = jax.random.split(jax.random.fold_in(streams_of[12], 1), IMG // ENC_DEV)
    dest_owner_turns = jax.random.permutation(jax.random.fold_in(streams_of[12], 3), IMG // ENC_DEV)
    dest_owner = jax.vmap(lambda own, number: deal_out(jax.random.fold_in(streams_of[12], 2), own, number, ENC_DEV, OWNERS, 1, CAP, 2))(dest_owner_keys, dest_owner_turns).reshape((IMG, 1))
    seq_length = touch_ends(jax.random.randint(streams_of[13], (OWNERS,), N_DP * CAP, LLM_DEV + 1), jax.random.fold_in(streams_of[13], 1), N_DP * CAP, LLM_DEV).astype(jnp.int32)
    return dict(hidden=hidden, enc_weight=enc_weight, enc_bias=enc_bias, enc_frozen=enc_frozen, enc_adapter=enc_adapter, text_rows=text_rows, norm_gain=norm_gain, value_weight=value_weight, value_bias=value_bias, llm_frozen=llm_frozen, llm_adapter=llm_adapter, targets=targets, dest_owner=dest_owner, seq_length=seq_length)


epsilon = 1e-06

def reference(hidden, enc_weight, enc_bias, enc_frozen, enc_adapter, text_rows, norm_gain, value_weight, value_bias, llm_frozen, llm_adapter, targets, dest_owner, seq_length):
    owners = N_DP * N_MP
    enc_low = jnp.dot(hidden, enc_frozen, preferred_element_type=jnp.float32).astype(jnp.bfloat16)
    merged_rows = jnp.dot(hidden, enc_weight, preferred_element_type=jnp.float32) + enc_bias.astype(jnp.float32)
    merged_rows = (merged_rows + jnp.dot(enc_low, enc_adapter, preferred_element_type=jnp.float32)).astype(jnp.bfloat16)
    destiny = dest_owner[:, 0].reshape(N_DP, ENC_DEV)
    markers = (destiny[:, :, None] == jnp.arange(owners, dtype=jnp.int32)[None, None, :]).astype(jnp.int32)
    slot_rank = lax.optimization_barrier(jnp.sum((jnp.cumsum(markers, axis=1) - markers) * markers, axis=2))
    placing = destiny * LLM_DEV + slot_rank * N_DP + jnp.arange(N_DP, dtype=jnp.int32)[:, None]
    placing = placing.reshape(-1).astype(jnp.int32)
    all_rows = text_rows.at[placing].set(merged_rows)
    wide_rows = all_rows.astype(jnp.float32)
    inverse = lax.rsqrt(lax.optimization_barrier(jnp.mean(wide_rows * wide_rows, axis=1, keepdims=True)) + epsilon)
    gain_wide = norm_gain.astype(jnp.float32)
    normed = (wide_rows * inverse * gain_wide).astype(jnp.bfloat16)
    low_rank = jnp.dot(normed, llm_frozen, preferred_element_type=jnp.float32).astype(jnp.bfloat16)
    values_out = jnp.dot(normed, value_weight, preferred_element_type=jnp.float32) + value_bias.astype(jnp.float32)
    values_out = values_out + jnp.dot(low_rank, llm_adapter, preferred_element_type=jnp.float32)
    position = jnp.arange(owners * LLM_DEV, dtype=jnp.int32) % LLM_DEV
    length = jnp.repeat(seq_length, LLM_DEV)
    row_weight = jnp.where(position < length, 1.0 / length.astype(jnp.float32), 0.0).astype(jnp.float32)
    dvalues = ((values_out - targets.astype(jnp.float32)) * row_weight[:, None]).astype(jnp.bfloat16)
    grad_llm = jnp.dot(low_rank.T, dvalues, preferred_element_type=jnp.float32)
    low_grad = jnp.dot(dvalues, llm_adapter.T, preferred_element_type=jnp.float32).astype(jnp.bfloat16)
    picked_dv = dvalues[placing]
    picked_low = low_grad[placing]
    picked_rows = wide_rows[placing]
    picked_inverse = inverse[placing]
    dnormed = jnp.dot(picked_dv, value_weight.T, preferred_element_type=jnp.float32)
    dnormed = dnormed + jnp.dot(picked_low, llm_frozen.T, preferred_element_type=jnp.float32)
    scaled = gain_wide * dnormed
    cubed = picked_inverse * picked_inverse * picked_inverse
    image_grad = picked_inverse * scaled - picked_rows * cubed * lax.optimization_barrier(jnp.mean(scaled * picked_rows, axis=1, keepdims=True))
    image_grad = image_grad.astype(jnp.bfloat16)
    grad_enc = jnp.dot(enc_low.T, image_grad, preferred_element_type=jnp.float32)
    return (grad_enc, grad_llm)
```

```python
import functools

import jax
import jax.numpy as jnp
from jax import lax
from jax.experimental import pallas as pl
from jax.experimental.pallas import tpu as pltpu
from jax.sharding import PartitionSpec as P

epsilon = 1e-06
F32 = jnp.float32
BF16 = jnp.bfloat16
MESH = pl.DeviceIdType.MESH
NN = (((1,), (0,)), ((), ()))
NT = (((1,), (1,)), ((), ()))


def dot(a, b, dims=NN):
    return lax.dot_general(a, b, dims, preferred_element_type=F32)


def split(x):
    high = x.astype(BF16)
    rest = (x - high.astype(F32)).astype(BF16)
    return jnp.concatenate([high, rest], axis=0)


def joined(x):
    half = x.shape[0] // 2
    return x[:half] + x[half:]


def eye(n):
    return (
        lax.broadcasted_iota(jnp.int32, (n, n), 0) == lax.broadcasted_iota(jnp.int32, (n, n), 1)
    ).astype(BF16)


def kernel(
    sizes,
    hidden, enc_weight, enc_bias, enc_frozen, enc_adapter, text_rows, gain_ref, value_weight,
    bias_ref, llm_frozen, adapter_ref, targets, dest, seq_length,
    out_enc, out_llm,
    ebuf, hid, acc, acc_low, img, xq, xr, wq, at, txt, gs, gr, tgs, tgr, los, lor,
    vown, vps, vpr, vs, vr, ys, yr, yrs, yrr, ss, sr, hys, hyr, hbs, hb, yos, s2s, s2r, fo,
    e_sem, t_sem, own_sem, h_ss, h_rs, hf_ss, hf_rs, w_ss, w_rs, a1_ss, a1_rs, a2_ss, a2_rs,
    a3_ss, a3_rs, tg_ss, tg_rs, x_ss, x_rs, lo_ss, lo_rs, g_ss, g_rs, vp_ss, vp_rs, v_ss, v_rs,
    yp_ss, yp_rs, yr_ss, yr_rs, s_ss, s_rs, hy_ss, hy_rs, hb_ss, hb_rs, yo_ss, yo_rs,
    s2_ss, s2_rs, fo_ss, fo_rs,
):
    z = sizes
    DP, MP = z["DP"], z["MP"]
    NTOK, BT, CAP, ST, LR = z["NTOK"], z["BT"], z["CAP"], z["ST"], z["LR"]
    D, MH, RANK, KV, NB = z["D"], z["MH"], z["RANK"], z["KV"], z["NB"]
    SH, HC, Q, R, UN, RU, RD, RG, KC = (z[k] for k in ("SH", "HC", "Q", "R", "UN", "RU", "RD", "RG", "KC"))
    KH = KV // 2
    NK = MH // KC
    QB = Q // R
    OWN = DP * MP
    c = lax.axis_index("grp")
    e = lax.axis_index("dp")
    m = lax.axis_index("mp")
    p, u = e % 2, e // 2
    oc = 1 - c
    t0 = (p + m // 2 + c) % 2
    owner = e * MP + m
    pending = []

    def copy(src, dst, ssem, rsem, dp=None, mp=None, grp=None):
        device = {"grp": c if grp is None else grp, "dp": e if dp is None else dp, "mp": m if mp is None else mp}
        return pltpu.make_async_remote_copy(
            src_ref=src, dst_ref=dst, send_sem=ssem, recv_sem=rsem, device_id=device, device_id_type=MESH
        )

    def send(*args, **kw):
        made = copy(*args, **kw)
        made.start()
        pending.append(made)

    def landed(dst, ssem, rsem):
        copy(dst, dst, ssem, rsem, grp=oc).wait_recv()

    half = c * HC
    loads = []
    for k in range(NK):
        one = pltpu.make_async_copy(
            enc_weight.at[pl.ds(k * KC, KC), pl.ds(half, HC)], ebuf.at[pl.ds(k * KC, KC), :], e_sem.at[k]
        )
        loads.append(one)
    text_load = pltpu.make_async_copy(text_rows, txt, t_sem)
    own_load = pltpu.make_async_copy(hidden, hid.at[pl.ds(m * NTOK, NTOK), :], own_sem)
    own_load.start()
    text_load.start()
    for one in loads:
        one.start()

    RH = RANK // 2
    low_half = c * RH
    at_own = dot(eye(RANK), llm_frozen[...], NT).astype(BF16)
    at[e, m, pl.ds(low_half, RH), :] = jnp.where(c == 0, at_own[:RH], at_own[RH:])
    rows = CAP * DP
    order_i = lax.broadcasted_iota(jnp.int32, (rows, rows), 0)
    order_j = lax.broadcasted_iota(jnp.int32, (rows, rows), 1)
    order = (order_j == order_i % CAP * DP + order_i // CAP).astype(BF16)
    sorted_targets = dot(order, targets[pl.ds(0, rows), pl.ds(c * KH, KH)]).astype(BF16)
    length = seq_length[...].astype(F32)
    for i in range(DP):
        for j in range(MP):
            block = sorted_targets[i * CAP : (i + 1) * CAP, j * NB : (j + 1) * NB]
            tail = jnp.broadcast_to(length, (ST - CAP, NB)).astype(BF16)
            tgs[i, j] = jnp.concatenate([block, tail], axis=0)

    barrier = pltpu.get_barrier_semaphore()
    devices = 2 * OWN
    place = (c * DP + e) * MP + m

    def greet(i, carry):
        other = (place + i) % devices
        device = {"grp": other // OWN, "dp": other // MP % DP, "mp": other % MP}
        pl.semaphore_signal(barrier, inc=1, device_id=device, device_id_type=MESH)
        return carry

    lax.fori_loop(1, devices, greet, 0)
    pl.semaphore_wait(barrier, devices - 1)

    for i in range(1, DP):
        mine = at.at[e, m, pl.ds(low_half, RH), :]
        send(mine, mine, a1_ss.at[i], a1_rs.at[i], dp=(e + i) % DP)
    NH = NTOK // 2
    hid_rows = pl.ds(m * NTOK + c * NH, NH)
    for k in range(NK):
        cols = pl.ds(k * KC, KC)
        for i in range(1, MP):
            send(hidden.at[pl.ds(c * NH, NH), cols], hid.at[hid_rows, cols], h_ss.at[k, i], h_rs.at[k, i], mp=(m + i) % MP)
    w_row = owner * R
    w_m = w_row // SH
    w_t = w_row % SH // Q
    w_slot = w_row % Q // R
    w_core = w_t // 2
    w_par = (w_t % 2 + w_t // 2 + w_m // 2) % 2
    w_sends = []
    for i in range((UN + 1) // 2):
        w_u = 2 * i + c
        there = 2 * w_u + w_par
        self_case = (there == e) & (w_m == m) & (w_core == c)
        live = w_u < UN
        away = copy(value_weight, wq.at[w_slot], w_ss.at[i], w_rs.at[w_slot], dp=there, mp=w_m, grp=w_core)
        near = pltpu.make_async_copy(value_weight, wq.at[w_slot], w_rs.at[w_slot])
        w_sends.append((live & jnp.logical_not(self_case), away))

        @pl.when(live & jnp.logical_not(self_case))
        def _():
            away.start()

        @pl.when(live & self_case)
        def _():
            near.start()

    for i in range(1, OWN):
        other = (owner + i) % OWN
        od, om = other // MP, other % MP
        send(tgs.at[od, om], tgr.at[e, m], tg_ss.at[i], tg_rs.at[i], dp=od, mp=om)
    tgr[e, m] = tgs[e, m]

    text_load.wait()
    TR = 16
    CW = min(D, 1024)

    def text_norm(i, carry):
        r = pl.ds(i * TR, TR)
        total = jnp.zeros((TR, 128), F32)
        for k in range(D // CW):
            part = txt[r, pl.ds(k * CW, CW)].astype(F32)
            part = part * part
            for n in range(CW // 128):
                total = total + part[:, n * 128 : (n + 1) * 128]
        inverse = lax.rsqrt(jnp.sum(total, axis=1, keepdims=True) / D + epsilon)
        for k in range(D // CW):
            cols = pl.ds(k * CW, CW)
            txt[r, cols] = (txt[r, cols].astype(F32) * inverse * gain_ref[:, cols].astype(F32)).astype(BF16)
        return carry

    lax.fori_loop(0, LR // TR, text_norm, 0)

    for i in range(1, DP):
        there = at.at[(e + DP - i) % DP, m, pl.ds(low_half, RH), :]
        landed(there, a1_ss.at[i], a1_rs.at[i])
    for i in range(1, MP):
        mine = at.at[:, m, pl.ds(low_half, RH), :]
        send(mine, mine, a2_ss.at[i], a2_rs.at[i], mp=(m + i) % MP)

    own_load.wait()
    TN = min(HC, 256)
    for k in range(NK):
        cols = pl.ds(k * KC, KC)
        for i in range(1, MP):
            peer = (m + MP - i) % MP
            there = hid.at[pl.ds(peer * NTOK + c * NH, NH), cols]
            landed(there, h_ss.at[k, i], h_rs.at[k, i])
            send(there, there, hf_ss.at[k, i], hf_rs.at[k, i], grp=oc)
        loads[k].wait()
        for i in range(1, MP):
            peer = (m + MP - i) % MP
            there = hid.at[pl.ds(peer * NTOK + oc * NH, NH), cols]
            landed(there, hf_ss.at[k, i], hf_rs.at[k, i])

        def product(n, carry):
            part = dot(hid[:, cols], ebuf[cols, pl.ds(n * TN, TN)])
            if k == 0:
                acc[:, pl.ds(n * TN, TN)] = part
            else:
                acc[:, pl.ds(n * TN, TN)] += part
            return carry

        lax.fori_loop(0, HC // TN, product, 0)
        low_part = dot(hid[:, cols], enc_frozen[cols, :])
        if k == 0:
            acc_low[...] = low_part
        else:
            acc_low[...] += low_part
    enc_low = acc_low[...].astype(BF16)
    enc_low_t = dot(eye(RANK), enc_low, NT)
    squares = jnp.zeros((BT, 128), F32)
    for n in range(HC // TN):
        cols = pl.ds(n * TN, TN)
        shifted = pl.ds(half + n * TN, TN)
        merged = acc[:, cols] + enc_bias[:, shifted].astype(F32) + dot(enc_low, enc_adapter[:, shifted])
        merged = merged.astype(BF16)
        img[:, cols] = merged
        wide = merged.astype(F32)
        square = wide * wide
        for i in range(TN // 128):
            squares = squares + square[:, i * 128 : (i + 1) * 128]
        scaled = (wide * gain_ref[:, pl.ds(m * SH + half + n * TN, TN)].astype(F32)).astype(BF16)
        xq[n * TN // Q, :, n * TN % Q : n * TN % Q + TN] = scaled
    pair = e + 1 - 2 * p
    send(xq.at[1 - t0], xr, x_ss, x_rs, dp=pair)

    for i in range(1, MP):
        there = at.at[:, (m + MP - i) % MP, pl.ds(low_half, RH), :]
        landed(there, a2_ss.at[i], a2_rs.at[i])
    mine = at.at[:, :, pl.ds(low_half, RH), :]
    send(mine, mine, a3_ss, a3_rs, grp=oc)
    landed(at.at[:, :, pl.ds(oc * RH, RH), :], a3_ss, a3_rs)

    first = (m * SH + half) // R
    low_part = jnp.zeros((RANK, BT), F32)
    for i in range(HC // R):
        q = first + i
        x = xq[i * R // Q, :, i * R % Q : i * R % Q + R]
        low_part = low_part + dot(at[q // MP, q % MP], x, NT)
    total = jnp.broadcast_to(jnp.sum(squares, axis=1, keepdims=True), (BT, 128))
    los[...] = jnp.concatenate([low_part, total.T[:8]], axis=0)
    me8 = m * 2 + c
    for i in range(1, 2 * MP):
        other = (me8 + i) % (2 * MP)
        send(los, lor.at[me8], lo_ss.at[i], lo_rs.at[i], mp=other // 2, grp=other % 2)
    lor[me8] = los[...]

    def text_low(q, carry):
        lt, ln = carry
        part = txt[:, pl.ds(pl.multiple_of(q * R, 128), R)]
        a = at[q // MP, q % MP]
        return lt + dot(a, part, NT), ln + dot(part, a, NT)

    text_low_t, text_low_n = lax.fori_loop(
        0, OWN, text_low, (jnp.zeros((RANK, LR), F32), jnp.zeros((LR, RANK), F32))
    )
    place_row = lax.broadcasted_iota(jnp.int32, (8, LR), 1)
    count = jnp.zeros((8, LR), F32)
    for i in range(DP):
        named = (dest[pl.ds(i * BT, BT), :] == owner).astype(F32)
        named = jnp.sum(named, axis=0, keepdims=True)
        count = jnp.where(place_row % DP == i, jnp.broadcast_to(named, (8, LR)), count)
    replaced = (place_row < CAP * DP) & ((place_row // DP).astype(F32) < count)
    live = (place_row.astype(F32) < jnp.broadcast_to(length, (8, LR))) & jnp.logical_not(replaced)
    live = jnp.where(live, 1.0, 0.0)[:1]
    text_low_m = (text_low_t.astype(BF16).astype(F32) * live).astype(BF16)
    text_low_b = text_low_n.astype(BF16)
    scale = 1.0 / length
    here8 = p * MP + m
    for j in range(MP):
        for i in range(2):
            col = pl.multiple_of(j * SH + half + i * Q, 128)
            gs[j, i] = (dot(text_low_m, txt[:, pl.ds(col, Q)]) * scale).astype(BF16)
    for i in range(1, 2 * MP):
        other = (here8 + i) % (2 * MP)
        gp, gm = other // MP, other % MP
        send(gs.at[gm, (gp + gm // 2 + c) % 2], gr.at[p, m], g_ss.at[i], g_rs.at[i], dp=2 * u + gp, mp=gm)
    gr[p, m] = gs[m, t0]
    text_y = dot(text_low_b, adapter_ref[:, pl.ds(c * KH, KH)])
    text_y = text_y + bias_ref[:, pl.ds(c * KH, KH)].astype(F32) - targets[:, pl.ds(c * KH, KH)].astype(F32)
    high = text_y.astype(BF16)
    rest = (text_y - high.astype(F32)).astype(BF16)
    text_grad = (dot(text_low_m, high) + dot(text_low_m, rest)) * scale

    for i in range(1, OWN):
        other = (owner + OWN - i) % OWN
        landed(tgr.at[other // MP, other % MP], tg_ss.at[i], tg_rs.at[i])
    block_dest = dest[pl.ds(pl.multiple_of(e * BT, 8), BT), :]
    marks = block_dest == lax.broadcasted_iota(jnp.int32, (BT, 128), 1)
    before = lax.broadcasted_iota(jnp.int32, (BT, BT), 0) > lax.broadcasted_iota(jnp.int32, (BT, BT), 1)
    counted = dot(before.astype(BF16), marks.astype(BF16))
    slot = jnp.sum(jnp.where(marks, counted, 0.0), axis=1, keepdims=True)
    base = block_dest.astype(F32) * ST
    table_rows = lax.broadcasted_iota(jnp.int32, (BT, OWN * ST), 1).astype(F32)
    table = tgr[...].reshape(OWN * ST, NB)
    image_targets = dot((table_rows == base + slot).astype(BF16), table)
    image_length = dot((table_rows == base + CAP).astype(BF16), table)
    position = slot * DP + e.astype(F32)
    weight = jnp.where(position < image_length, 1.0 / image_length, 0.0)

    gathered = jnp.zeros((RANK + 8, BT), F32)
    for i in range(1, 2 * MP):
        other = (me8 + 2 * MP - i) % (2 * MP)
        landed(lor.at[other], lo_ss.at[i], lo_rs.at[i])
    for i in range(2 * MP):
        gathered = gathered + lor[i]
    inverse_row = lax.rsqrt(gathered[RANK : RANK + 1] / D + epsilon)
    low_t = (gathered[:RANK] * inverse_row).astype(BF16)
    turned = jnp.concatenate(
        [low_t.astype(F32), jnp.broadcast_to(inverse_row, (128 - RANK, BT))], axis=0
    ).T
    low = turned[:, :RANK].astype(BF16)
    inverse = turned[:, RANK : RANK + 1]

    for i in range(QB):
        landed(wq.at[i], w_ss.at[0], w_rs.at[i])

    def values_of(x, where, first_col):
        for n in range(KH // TN):
            cols = pl.ds(pl.multiple_of(first_col + n * TN, 128), TN)
            part = dot(x[:, :R], wq[0, :, cols])
            for i in range(1, QB):
                part = part + dot(x[:, i * R : (i + 1) * R], wq[i, :, cols])
            where[:, n * TN : (n + 1) * TN] = part.astype(where.dtype)

    values_of(xq[t0], vps.at[p], oc * KH)
    send(vps.at[p], vpr.at[p], vp_ss.at[0], vp_rs.at[0], grp=oc)
    landed(xr, x_ss, x_rs)
    values_of(xr[...], vps.at[1 - p], oc * KH)
    send(vps.at[1 - p], vpr.at[1 - p], vp_ss.at[1], vp_rs.at[1], grp=oc)
    values_of(xq[t0], vown.at[p], c * KH)
    values_of(xr[...], vown.at[1 - p], c * KH)
    landed(vpr.at[p], vp_ss.at[0], vp_rs.at[0])
    landed(vpr.at[1 - p], vp_ss.at[1], vp_rs.at[1])
    for i in range(2):
        both = (vown[i] + vpr[i].astype(F32)).astype(BF16)
        for j in range(MP):
            vs[i, j] = both[:, j * NB : (j + 1) * NB]
    for i in range(1, 2 * MP):
        other = (here8 + i) % (2 * MP)
        gp, gm = other // MP, other % MP
        send(vs.at[gp, gm], vr.at[p, m], v_ss.at[i], v_rs.at[i], dp=2 * u + gp, mp=gm)
    vr[p, m] = vs[p, m]

    for i in range(1, 2 * MP):
        other = (here8 + 2 * MP - i) % (2 * MP)
        landed(gr.at[other // MP, other % MP], g_ss.at[i], g_rs.at[i])
    g_sum = jnp.zeros((RANK, Q), F32)
    for i in range(2):
        for j in range(MP):
            g_sum = g_sum + gr[i, j].astype(F32)
    g_pair = split(g_sum)

    def through(cols):
        part = dot(g_pair[:, :R], wq[0, :, cols])
        for i in range(1, QB):
            part = part + dot(g_pair[:, i * R : (i + 1) * R], wq[i, :, cols])
        return joined(part)

    ys[...] = through(pl.ds(oc * KH, KH))
    send(ys, yr, yp_ss, yp_rs, grp=oc)
    text_grad = text_grad + through(pl.ds(c * KH, KH))
    landed(yr, yp_ss, yp_rs)
    text_grad = text_grad + yr[...]
    for i in range(DP):
        for j in range(MP):
            yrs[i, j] = text_grad[i * RD : (i + 1) * RD, j * NB : (j + 1) * NB]
    for i in range(1, OWN):
        other = (owner + i) % OWN
        od, om = other // MP, other % MP
        send(yrs.at[od, om], yrr.at[e, m], yr_ss.at[i], yr_rs.at[i], dp=od, mp=om)
    yrr[e, m] = yrs[e, m]

    for i in range(1, 2 * MP):
        other = (here8 + 2 * MP - i) % (2 * MP)
        landed(vr.at[other // MP, other % MP], v_ss.at[i], v_rs.at[i])
    product_sum = jnp.zeros((BT, NB), F32)
    for i in range(2):
        for j in range(MP):
            product_sum = product_sum + vr[i, j].astype(F32)
    own_cols = pl.ds(pl.multiple_of(c * KH + m * NB, 128), NB)
    plain = product_sum * inverse + dot(low, adapter_ref[:, own_cols])
    dv = plain + bias_ref[:, own_cols].astype(F32) - image_targets
    dv = (dv * weight).astype(BF16)
    along = jnp.sum(dv.astype(F32) * plain, axis=1, keepdims=True)
    ss[...] = jnp.broadcast_to(along, (BT, 128)).T[:8]
    for i in range(1, 2 * MP):
        other = (me8 + i) % (2 * MP)
        send(ss, sr.at[me8], s_ss.at[i], s_rs.at[i], mp=other // 2, grp=other % 2)
    sr[me8] = ss[...]
    h_part = joined(dot(split(enc_low_t * inverse_row), dv))
    y_part = dot(low_t, dv)
    for i in range(DP):
        hys[i, 0] = h_part[i * RD : (i + 1) * RD]
        hys[i, 1] = y_part[i * RD : (i + 1) * RD]
    for i in range(1, DP):
        there = (e + i) % DP
        send(hys.at[there], hyr.at[e], hy_ss.at[i], hy_rs.at[i], dp=there)
    hyr[e] = hys[e]

    for i in range(1, 2 * MP):
        other = (me8 + 2 * MP - i) % (2 * MP)
        landed(sr.at[other], s_ss.at[i], s_rs.at[i])
    along_row = jnp.zeros((8, BT), F32)
    for i in range(2 * MP):
        along_row = along_row + sr[i]
    factor = along_row[:1] * inverse_row * inverse_row / D
    second_pair = split(enc_low_t * factor)
    for i in range(2):
        second = joined(dot(second_pair, img[:, pl.ds(i * Q, Q)])).astype(BF16)
        for j in range(UN):
            s2s[i, j] = second[j * RU : (j + 1) * RU]
    for i in range(1, DP):
        there = (e + i) % DP
        send(s2s.at[(there % 2 + c + m // 2) % 2, there // 2], s2r.at[e], s2_ss.at[i], s2_rs.at[i], dp=there)
    s2r[e] = s2s[t0, u]

    for i in range(1, DP):
        landed(hyr.at[(e + DP - i) % DP], hy_ss.at[i], hy_rs.at[i])
    hy = hyr[0]
    for i in range(1, DP):
        hy = hy + hyr[i]
    hbs[...] = hy[0]
    unit = (p * 2 + c) * MP + m
    for i in range(1, 4 * MP):
        other = (unit + i) % (4 * MP)
        send(
            hbs, hb.at[p, c, m], hb_ss.at[i], hb_rs.at[i],
            dp=2 * u + other // (2 * MP), grp=other // MP % 2, mp=other % MP,
        )
    hb[p, c, m] = hbs[...]
    for i in range(1, OWN):
        other = (owner + OWN - i) % OWN
        landed(yrr.at[other // MP, other % MP], yr_ss.at[i], yr_rs.at[i])
    y_sum = hy[1]
    for i in range(DP):
        for j in range(MP):
            y_sum = y_sum + yrr[i, j]
    yos[...] = y_sum
    DH = DP // 2
    y_core = e // DH
    y_row = e % DH
    y_there = out_llm.at[y_row, :, own_cols]
    for i in range(1, OWN):
        other = (owner + i) % OWN
        send(yos, y_there, yo_ss.at[i], yo_rs.at[y_row, m, c], dp=other // MP, mp=other % MP, grp=y_core)
    y_away = copy(yos, y_there, yo_ss.at[0], yo_rs.at[y_row, m, c], grp=oc)

    @pl.when(y_core == c)
    def _():
        out_llm[y_row, :, own_cols] = yos[...]

    @pl.when(y_core != c)
    def _():
        y_away.start()

    for i in range(1, 4 * MP):
        other = (unit + 4 * MP - i) % (4 * MP)
        landed(hb.at[other // (2 * MP), other // MP % 2, other % MP], hb_ss.at[i], hb_rs.at[i])
    h_all = jnp.concatenate(
        [
            jnp.concatenate([hb[i, j, k] for j in range(2) for k in range(MP)], axis=1)
            for i in range(2)
        ],
        axis=0,
    )
    h_pair = split(h_all)
    h_low = split(joined(dot(h_pair, adapter_ref[...], NT)))
    quarter = m * SH + half + t0 * Q
    parts = []
    for i in range(QB):
        q = quarter // R + i
        part = joined(dot(h_pair, wq[i], NT)) + joined(dot(h_low, at[q // MP, q % MP]))
        parts.append(part * gain_ref[:, pl.ds(pl.multiple_of(quarter + i * R, 128), R)].astype(F32))
    result = jnp.concatenate(parts, axis=1)
    for i in range(1, DP):
        landed(s2r.at[(e + DP - i) % DP], s2_ss.at[i], s2_rs.at[i])
    for i in range(DP):
        result = result - s2r[i].astype(F32)
    fo[...] = result
    UH = UN // 2
    f_core = u // UH
    f_unit = u % UH
    f_cols = pl.ds(pl.multiple_of(half + t0 * Q, 128), Q)
    f_there = out_enc.at[pl.ds(pl.multiple_of(f_unit * RU, 8), RU), f_cols]
    for i in range(1, DP):
        send(fo, f_there, fo_ss.at[i], fo_rs.at[f_unit, p, c], dp=(e + i) % DP, grp=f_core)
    f_away = copy(fo, f_there, fo_ss.at[0], fo_rs.at[f_unit, p, c], grp=oc)

    @pl.when(f_core == c)
    def _():
        out_enc[pl.ds(pl.multiple_of(f_unit * RU, 8), RU), f_cols] = fo[...]

    @pl.when(f_core != c)
    def _():
        f_away.start()

    for i in range(DH):
        for j in range(MP):
            for k in range(2):
                other = copy(yos, out_llm.at[i, :, pl.ds(k * KH + j * NB, NB)], yo_ss.at[0], yo_rs.at[i, j, k], grp=oc)

                @pl.when(jnp.logical_not((y_core == c) & (y_row == i) & (m == j) & (c == k)))
                def _():
                    other.wait_recv()

    for i in range(UH):
        for j in range(2):
            for k in range(2):
                t_other = (j + m // 2 + k) % 2
                cols = pl.ds(pl.multiple_of(k * HC + t_other * Q, 128), Q)
                arrival = copy(fo, out_enc.at[pl.ds(i * RU, RU), cols], fo_ss.at[0], fo_rs.at[i, j, k], grp=oc)

                @pl.when(jnp.logical_not((f_core == c) & (f_unit == i) & (p == j) & (c == k)))
                def _():
                    arrival.wait_recv()

    for one in pending:
        one.wait_send()
    for started, one in w_sends:

        @pl.when(started)
        def _():
            one.wait_send()

    @pl.when(y_core != c)
    def _():
        y_away.wait_send()

    @pl.when(f_core != c)
    def _():
        f_away.wait_send()


def body(
    hidden, enc_weight, enc_bias, enc_frozen, enc_adapter, text_rows, norm_gain, value_weight,
    value_bias, llm_frozen, llm_adapter, targets, dest_owner, seq_length,
):
    DP, MP = lax.axis_size("dp"), lax.axis_size("mp")
    OWN = DP * MP
    NTOK, MH = hidden.shape
    BT = NTOK * MP
    LR, D = text_rows.shape
    RANK = enc_frozen.shape[1]
    KV = llm_adapter.shape[1]
    CAP = 2 * BT // OWN
    ST = CAP + 8
    ST = ST + -ST % 16
    SH = enc_weight.shape[1]
    HC, Q = SH // 2, SH // 4
    R = value_weight.shape[0]
    UN = DP // 2
    RU, RD, RG = RANK // UN, RANK // DP, RANK // 2
    KH, NB = KV // 2, KV // (2 * MP)
    KC = 1024 if MH % 1024 == 0 else MH
    NK = MH // KC
    QB = Q // R
    RL = RANK + 8
    sizes = dict(
        DP=DP, MP=MP, NTOK=NTOK, BT=BT, CAP=CAP, ST=ST, LR=LR, D=D, MH=MH, RANK=RANK, KV=KV, NB=NB,
        SH=SH, HC=HC, Q=Q, R=R, UN=UN, RU=RU, RD=RD, RG=RG, KC=KC,
    )
    vmem = pl.BlockSpec(memory_space=pltpu.VMEM)
    hbm = pl.BlockSpec(memory_space=pl.ANY)
    V = pltpu.VMEM
    S = pltpu.SemaphoreType.DMA
    scratch = [
        V((MH, HC), BF16), V((BT, MH), BF16), V((BT, HC), F32), V((BT, RANK), F32), V((BT, HC), BF16),
        V((2, BT, Q), BF16), V((BT, Q), BF16), V((QB, R, KV), BF16), V((DP, MP, RANK, R), BF16), V((LR, D), BF16),
        V((MP, 2, RANK, Q), BF16), V((2, MP, RANK, Q), BF16), V((DP, MP, ST, NB), BF16), V((DP, MP, ST, NB), BF16),
        V((RL, BT), F32), V((2 * MP, RL, BT), F32),
        V((2, BT, KH), F32), V((2, BT, KH), BF16), V((2, BT, KH), BF16),
        V((2, MP, BT, NB), BF16), V((2, MP, BT, NB), BF16),
        V((RANK, KH), F32), V((RANK, KH), F32), V((DP, MP, RD, NB), F32), V((DP, MP, RD, NB), F32),
        V((8, BT), F32), V((2 * MP, 8, BT), F32), V((DP, 2, RD, NB), F32), V((DP, 2, RD, NB), F32),
        V((RD, NB), F32), V((2, 2, MP, RD, NB), F32), V((RD, NB), F32),
        V((2, UN, RU, Q), BF16), V((DP, RU, Q), BF16), V((RU, Q), F32),
        S((NK,)), S(()), S(()), S((NK, MP)), S((NK, MP)), S((NK, MP)), S((NK, MP)),
        S(((UN + 1) // 2,)), S((QB,)), S((DP,)), S((DP,)), S((MP,)), S((MP,)),
        S(()), S(()), S((OWN,)), S((OWN,)), S(()), S(()), S((2 * MP,)), S((2 * MP,)), S((2 * MP,)), S((2 * MP,)),
        S((2,)), S((2,)), S((2 * MP,)), S((2 * MP,)),
        S(()), S(()), S((OWN,)), S((OWN,)), S((2 * MP,)), S((2 * MP,)), S((DP,)), S((DP,)),
        S((4 * MP,)), S((4 * MP,)), S((OWN,)), S((DP // 2, MP, 2)),
        S((DP,)), S((DP,)), S((DP,)), S((UN // 2, 2, 2)),
    ]
    grad_enc, grad_llm = pl.pallas_call(
        functools.partial(kernel, sizes),
        out_shape=(
            jax.ShapeDtypeStruct((RG, SH), F32),
            jax.ShapeDtypeStruct((DP // 2, RD, KV), F32),
        ),
        in_specs=[hbm, hbm, vmem, vmem, vmem, hbm, vmem, hbm, vmem, vmem, vmem, vmem, vmem, vmem],
        out_specs=(vmem, vmem),
        scratch_shapes=scratch,
        compiler_params=pltpu.CompilerParams(
            collective_id=0, has_side_effects=True, vmem_limit_bytes=60 * 1024 * 1024
        ),
    )(
        hidden, enc_weight, enc_bias.reshape(1, SH), enc_frozen, enc_adapter, text_rows,
        norm_gain.reshape(1, D), value_weight, value_bias.reshape(1, KV), llm_frozen, llm_adapter,
        targets, dest_owner, seq_length.reshape(1, 1),
    )
    return grad_enc, grad_llm.reshape(RG, KV)


def solution(mesh):
    return jax.shard_map(
        body,
        mesh=mesh,
        in_specs=(
            P(("dp", "mp"), None), P(None, "mp"), P("mp"), P(), P(None, "mp"), P(("dp", "mp"), None), P(),
            P(("dp", "mp"), None), P(), P(("dp", "mp"), None), P(), P(("dp", "mp"), None), P(), P(("dp", "mp")),
        ),
        out_specs=(P("grp", "mp"), P("grp", None)),
        check_vma=False,
    )
```

```python
import functools

import jax
import jax.numpy as jnp
from jax import lax
from jax.experimental import pallas as pl
from jax.experimental.pallas import tpu as pltpu
from jax.sharding import PartitionSpec as P

epsilon = 1e-06
F32 = jnp.float32
BF16 = jnp.bfloat16
MESH = pl.DeviceIdType.MESH
NN = (((1,), (0,)), ((), ()))
NT = (((1,), (1,)), ((), ()))


def dot(a, b, dims=NN):
    return lax.dot_general(a, b, dims, preferred_element_type=F32)


def split(x):
    high = x.astype(BF16)
    rest = (x - high.astype(F32)).astype(BF16)
    return jnp.concatenate([high, rest], axis=0)


def joined(x):
    half = x.shape[0] // 2
    return x[:half] + x[half:]


def eye(n):
    return (
        lax.broadcasted_iota(jnp.int32, (n, n), 0) == lax.broadcasted_iota(jnp.int32, (n, n), 1)
    ).astype(BF16)


def kernel(
    sizes,
    hidden, enc_weight, enc_bias_in, enc_frozen, enc_adapter, text_rows, gain_in, value_weight,
    bias_in, llm_frozen, adapter_ref, targets, dest, seq_length,
    out_enc, out_llm,
    gain_ref, enc_bias, bias_ref, ebuf, hid, acc, acc_low, img, xq, xr, wq, at, txt, gs, gr, tgs, tgr, los, lor,
    vown, vps, vpr, vs, vr, lop, ys, yr, yrs, yrr, ss, sr, hys, hyr, hbs, hb, yos, s2s, s2r, fo, fin,
    e_sem, t_sem, own_sem, h_ss, h_rs, hf_ss, hf_rs, w_ss, w_rs, lp_ss, lp_rs, a1_ss, a1_rs, a2_ss, a2_rs,
    a3_ss, a3_rs, tg_ss, tg_rs, x_ss, x_rs, lo_ss, lo_rs, g_ss, g_rs, vp_ss, vp_rs, v_ss, v_rs,
    yp_ss, yp_rs, yr_ss, yr_rs, s_ss, s_rs, hy_ss, hy_rs, hb_ss, hb_rs, yo_ss, yo_rs,
    s2_ss, s2_rs, fo_ss, fo_rs,
):
    z = sizes
    DP, MP = z["DP"], z["MP"]
    NTOK, BT, CAP, ST, LR = z["NTOK"], z["BT"], z["CAP"], z["ST"], z["LR"]
    D, MH, RANK, KV, NB = z["D"], z["MH"], z["RANK"], z["KV"], z["NB"]
    SH, HC, Q, R, UN, RU, RD, RG, KC = (z[k] for k in ("SH", "HC", "Q", "R", "UN", "RU", "RD", "RG", "KC"))
    KH = KV // 2
    NK = MH // KC
    QB = Q // R
    OWN = DP * MP
    c = lax.axis_index("grp")
    e = lax.axis_index("dp")
    m = lax.axis_index("mp")
    p, u = e % 2, e // 2
    oc = 1 - c
    t0 = (p + m // 2 + c) % 2
    owner = e * MP + m
    pending = []

    def copy(src, dst, ssem, rsem, dp=None, mp=None, grp=None):
        device = {"grp": c if grp is None else grp, "dp": e if dp is None else dp, "mp": m if mp is None else mp}
        return pltpu.make_async_remote_copy(
            src_ref=src, dst_ref=dst, send_sem=ssem, recv_sem=rsem, device_id=device, device_id_type=MESH
        )

    def send(*args, **kw):
        made = copy(*args, **kw)
        made.start()
        pending.append(made)

    def landed(dst, ssem, rsem):
        copy(dst, dst, ssem, rsem, grp=oc).wait_recv()

    barrier = pltpu.get_barrier_semaphore()
    devices = 2 * OWN
    place = (c * DP + e) * MP + m

    def greet(i, carry):
        other = (place + i) % devices
        device = {"grp": other // OWN, "dp": other // MP % DP, "mp": other % MP}
        pl.semaphore_signal(barrier, inc=1, device_id=device, device_id_type=MESH)
        return carry

    lax.fori_loop(1, devices, greet, 0)

    half = c * HC
    loads = []
    for k in range(NK):
        one = pltpu.make_async_copy(
            enc_weight.at[pl.ds(k * KC, KC), pl.ds(half, HC)], ebuf.at[pl.ds(k * KC, KC), :], e_sem.at[k]
        )
        loads.append(one)
    text_load = pltpu.make_async_copy(text_rows, txt, t_sem)
    own_load = pltpu.make_async_copy(hidden, hid.at[pl.ds(m * NTOK, NTOK), :], own_sem)
    own_load.start()
    text_load.start()
    for one in loads:
        one.start()

    RH = RANK // 2
    low_half = c * RH
    at[e, m, pl.ds(low_half, RH), :] = llm_frozen[pl.ds(pl.multiple_of(low_half, 16), RH), :]
    for packed, row in ((gain_in, gain_ref), (enc_bias_in, enc_bias), (bias_in, bias_ref)):
        wide = packed[...].astype(F32)
        for i in range(wide.shape[0]):
            row[:, i * 128 : (i + 1) * 128] = wide[i : i + 1]
    rows = CAP * DP
    order_i = lax.broadcasted_iota(jnp.int32, (rows, rows), 0)
    order_j = lax.broadcasted_iota(jnp.int32, (rows, rows), 1)
    order = (order_j == order_i % CAP * DP + order_i // CAP).astype(BF16)
    sorted_targets = dot(order, targets[pl.ds(0, rows), pl.ds(c * KH, KH)]).astype(BF16)
    length = seq_length[...].astype(F32)
    for i in range(DP):
        for j in range(MP):
            block = sorted_targets[i * CAP : (i + 1) * CAP, j * NB : (j + 1) * NB]
            tail = jnp.broadcast_to(length, (ST - CAP, NB)).astype(BF16)
            tgs[i, j] = jnp.concatenate([block, tail], axis=0)

    pl.semaphore_wait(barrier, devices - 1)

    w_sends = []

    def send_weights():
        w_row = owner * R
        w_m = w_row // SH
        w_t = w_row % SH // Q
        w_slot = w_row % Q // R
        w_core = w_t // 2
        w_par = (w_t % 2 + w_t // 2 + w_m // 2) % 2
        for i in range((UN + 1) // 2):
            w_u = 2 * i + c
            there = 2 * w_u + w_par
            self_case = (there == e) & (w_m == m) & (w_core == c)
            live = w_u < UN
            away = copy(value_weight, wq.at[w_slot], w_ss.at[i], w_rs.at[w_slot], dp=there, mp=w_m, grp=w_core)
            near = pltpu.make_async_copy(value_weight, wq.at[w_slot], w_rs.at[w_slot])
            w_sends.append((live & jnp.logical_not(self_case), away))

            @pl.when(live & jnp.logical_not(self_case))
            def _():
                away.start()

            @pl.when(live & self_case)
            def _():
                near.start()

    for i in range(1, DP):
        mine = at.at[e, m, pl.ds(low_half, RH), :]
        send(mine, mine, a1_ss.at[i], a1_rs.at[i], dp=(e + i) % DP)
    NH = NTOK // 2
    hid_rows = pl.ds(m * NTOK + c * NH, NH)
    for k in range(NK):
        cols = pl.ds(k * KC, KC)
        for i in range(1, MP):
            send(hidden.at[pl.ds(c * NH, NH), cols], hid.at[hid_rows, cols], h_ss.at[k, i], h_rs.at[k, i], mp=(m + i) % MP)
    send_weights()
    for i in range(1, OWN):
        other = (owner + i) % OWN
        od, om = other // MP, other % MP
        send(tgs.at[od, om], tgr.at[e, m], tg_ss.at[i], tg_rs.at[i], dp=od, mp=om)
    tgr[e, m] = tgs[e, m]

    text_load.wait()
    TR = 16
    CW = min(D, 1024)

    def text_norm(i, carry):
        r = pl.ds(i * TR, TR)
        total = jnp.zeros((TR, 128), F32)
        for k in range(D // CW):
            part = txt[r, pl.ds(k * CW, CW)].astype(F32)
            part = part * part
            for n in range(CW // 128):
                total = total + part[:, n * 128 : (n + 1) * 128]
        inverse = lax.rsqrt(jnp.sum(total, axis=1, keepdims=True) / D + epsilon)
        for k in range(D // CW):
            cols = pl.ds(k * CW, CW)
            txt[r, cols] = (txt[r, cols].astype(F32) * inverse * gain_ref[:, cols]).astype(BF16)
        return carry

    lax.fori_loop(0, LR // TR, text_norm, 0)

    for i in range(1, DP):
        there = at.at[(e + DP - i) % DP, m, pl.ds(low_half, RH), :]
        landed(there, a1_ss.at[i], a1_rs.at[i])
    for i in range(1, MP):
        mine = at.at[:, m, pl.ds(low_half, RH), :]
        send(mine, mine, a2_ss.at[i], a2_rs.at[i], mp=(m + i) % MP)

    own_load.wait()
    TN = min(HC, 256)
    for k in range(NK):
        cols = pl.ds(k * KC, KC)
        for i in range(1, MP):
            peer = (m + MP - i) % MP
            there = hid.at[pl.ds(peer * NTOK + c * NH, NH), cols]
            landed(there, h_ss.at[k, i], h_rs.at[k, i])
            send(there, there, hf_ss.at[k, i], hf_rs.at[k, i], grp=oc)
        loads[k].wait()
        for i in range(1, MP):
            peer = (m + MP - i) % MP
            there = hid.at[pl.ds(peer * NTOK + oc * NH, NH), cols]
            landed(there, hf_ss.at[k, i], hf_rs.at[k, i])

        def product(n, carry):
            part = dot(hid[:, cols], ebuf[cols, pl.ds(n * TN, TN)])
            if k == 0:
                acc[:, pl.ds(n * TN, TN)] = part
            else:
                acc[:, pl.ds(n * TN, TN)] += part
            return carry

        lax.fori_loop(0, HC // TN, product, 0)
        low_part = dot(hid[:, cols], enc_frozen[:, cols], NT)
        if k == 0:
            acc_low[...] = low_part
        else:
            acc_low[...] += low_part
    enc_low = acc_low[...].astype(BF16)
    enc_low_t = dot(eye(RANK), enc_low, NT)
    squares = jnp.zeros((BT, 128), F32)
    for n in range(HC // TN):
        cols = pl.ds(n * TN, TN)
        shifted = pl.ds(half + n * TN, TN)
        merged = acc[:, cols] + enc_bias[:, shifted] + dot(enc_low, enc_adapter[:, shifted])
        merged = merged.astype(BF16)
        img[:, cols] = merged
        wide = merged.astype(F32)
        square = wide * wide
        for i in range(TN // 128):
            squares = squares + square[:, i * 128 : (i + 1) * 128]
        scaled = (wide * gain_ref[:, pl.ds(m * SH + half + n * TN, TN)]).astype(BF16)
        xq[n * TN // Q, :, n * TN % Q : n * TN % Q + TN] = scaled
    pair = e + 1 - 2 * p
    send(xq.at[1 - t0], xr, x_ss, x_rs, dp=pair)

    for i in range(1, MP):
        there = at.at[:, (m + MP - i) % MP, pl.ds(low_half, RH), :]
        landed(there, a2_ss.at[i], a2_rs.at[i])
    mine = at.at[:, :, pl.ds(low_half, RH), :]
    send(mine, mine, a3_ss, a3_rs, grp=oc)
    landed(at.at[:, :, pl.ds(oc * RH, RH), :], a3_ss, a3_rs)

    first = (m * SH + half) // R
    low_part = jnp.zeros((RANK, BT), F32)
    for i in range(HC // R):
        q = first + i
        x = xq[i * R // Q, :, i * R % Q : i * R % Q + R]
        low_part = low_part + dot(at[q // MP, q % MP], x, NT)
    total = jnp.broadcast_to(jnp.sum(squares, axis=1, keepdims=True), (BT, 128))
    los[...] = jnp.concatenate([low_part, total.T[:8]], axis=0)
    me8 = m * 2 + c
    send(los, lop, lp_ss, lp_rs, grp=oc)
    landed(lop, lp_ss, lp_rs)
    lor[m] = los[...] + lop[...]
    for i in range(1, MP):
        send(lor.at[m], lor.at[m], lo_ss.at[i], lo_rs.at[i], mp=(m + i) % MP)

    def text_low(q, carry):
        part = txt[:, pl.ds(pl.multiple_of(q * R, 128), R)]
        return carry + dot(part, at[q // MP, q % MP], NT)

    text_low_n = lax.fori_loop(0, OWN, text_low, jnp.zeros((LR, RANK), F32))
    text_low_b = text_low_n.astype(BF16)
    text_low_t = jnp.concatenate([text_low_b.astype(F32), jnp.zeros((LR, 128 - RANK), F32)], axis=1).T[:RANK]
    place_row = lax.broadcasted_iota(jnp.int32, (8, LR), 1)
    count = jnp.zeros((8, LR), F32)
    for i in range(DP):
        named = (dest[:, i * BT : (i + 1) * BT] == owner).astype(F32)
        named = jnp.sum(named, axis=1, keepdims=True)
        count = jnp.where(place_row % DP == i, jnp.broadcast_to(named, (8, LR)), count)
    replaced = (place_row < CAP * DP) & ((place_row // DP).astype(F32) < count)
    live = (place_row.astype(F32) < jnp.broadcast_to(length, (8, LR))) & jnp.logical_not(replaced)
    live = jnp.where(live, 1.0, 0.0)[:1]
    text_low_m = (text_low_t * live).astype(BF16)
    scale = 1.0 / length
    here8 = p * MP + m
    for j in range(MP):
        for i in range(2):
            col = pl.multiple_of(j * SH + half + i * Q, 128)
            gs[j, i] = (dot(text_low_m, txt[:, pl.ds(col, Q)]) * scale).astype(BF16)
    for i in range(1, 2 * MP):
        other = (here8 + i) % (2 * MP)
        gp, gm = other // MP, other % MP
        send(gs.at[gm, (gp + gm // 2 + c) % 2], gr.at[p, m], g_ss.at[i], g_rs.at[i], dp=2 * u + gp, mp=gm)
    gr[p, m] = gs[m, t0]
    text_y = dot(text_low_b, adapter_ref[:, pl.ds(c * KH, KH)])
    text_y = text_y + bias_ref[:, pl.ds(c * KH, KH)] - targets[:, pl.ds(c * KH, KH)].astype(F32)
    high = text_y.astype(BF16)
    rest = (text_y - high.astype(F32)).astype(BF16)
    text_grad = (dot(text_low_m, high) + dot(text_low_m, rest)) * scale

    for i in range(QB):
        landed(wq.at[i], w_ss.at[0], w_rs.at[i])

    def values_of(x, where, first_col):
        for n in range(KH // TN):
            cols = pl.ds(pl.multiple_of(first_col + n * TN, 128), TN)
            part = dot(x[:, :R], wq[0, :, cols])
            for i in range(1, QB):
                part = part + dot(x[:, i * R : (i + 1) * R], wq[i, :, cols])
            where[:, n * TN : (n + 1) * TN] = part.astype(where.dtype)

    values_of(xq[t0], vps.at[p], oc * KH)
    send(vps.at[p], vpr.at[p], vp_ss.at[0], vp_rs.at[0], grp=oc)
    landed(xr, x_ss, x_rs)
    values_of(xr[...], vps.at[1 - p], oc * KH)
    send(vps.at[1 - p], vpr.at[1 - p], vp_ss.at[1], vp_rs.at[1], grp=oc)
    values_of(xq[t0], vown.at[p], c * KH)
    values_of(xr[...], vown.at[1 - p], c * KH)
    landed(vpr.at[p], vp_ss.at[0], vp_rs.at[0])
    landed(vpr.at[1 - p], vp_ss.at[1], vp_rs.at[1])
    for i in range(2):
        both = (vown[i] + vpr[i].astype(F32)).astype(BF16)
        for j in range(MP):
            vs[i, j] = both[:, j * NB : (j + 1) * NB]
    for i in range(1, 2 * MP):
        other = (here8 + i) % (2 * MP)
        gp, gm = other // MP, other % MP
        send(vs.at[gp, gm], vr.at[p, m], v_ss.at[i], v_rs.at[i], dp=2 * u + gp, mp=gm)
    vr[p, m] = vs[p, m]

    for i in range(1, OWN):
        other = (owner + OWN - i) % OWN
        landed(tgr.at[other // MP, other % MP], tg_ss.at[i], tg_rs.at[i])
    block_dest = dest[:, pl.ds(pl.multiple_of(e * BT, 128), BT)].astype(F32)
    block_dest = jnp.broadcast_to(block_dest, (128, BT)).T
    marks = block_dest == lax.broadcasted_iota(jnp.int32, (BT, 128), 1).astype(F32)
    before = lax.broadcasted_iota(jnp.int32, (BT, BT), 0) > lax.broadcasted_iota(jnp.int32, (BT, BT), 1)
    counted = dot(before.astype(BF16), marks.astype(BF16))
    slot = jnp.sum(jnp.where(marks, counted, 0.0), axis=1, keepdims=True)
    base = block_dest[:, :1] * ST
    table_rows = lax.broadcasted_iota(jnp.int32, (BT, OWN * ST), 1).astype(F32)
    table = tgr[...].reshape(OWN * ST, NB)
    image_targets = dot((table_rows == base + slot).astype(BF16), table)
    image_length = dot((table_rows == base + CAP).astype(BF16), table)
    position = slot * DP + e.astype(F32)
    weight = jnp.where(position < image_length, 1.0 / image_length, 0.0)

    gathered = jnp.zeros((RANK + 8, BT), F32)
    for i in range(1, MP):
        landed(lor.at[(m + MP - i) % MP], lo_ss.at[i], lo_rs.at[i])
    for i in range(MP):
        gathered = gathered + lor[i]
    inverse_row = lax.rsqrt(gathered[RANK : RANK + 1] / D + epsilon)
    low_t = (gathered[:RANK] * inverse_row).astype(BF16)
    turned = jnp.concatenate(
        [low_t.astype(F32), jnp.broadcast_to(inverse_row, (128 - RANK, BT))], axis=0
    ).T
    low = turned[:, :RANK].astype(BF16)
    inverse = turned[:, RANK : RANK + 1]

    for i in range(1, 2 * MP):
        other = (here8 + 2 * MP - i) % (2 * MP)
        landed(vr.at[other // MP, other % MP], v_ss.at[i], v_rs.at[i])
    product_sum = jnp.zeros((BT, NB), F32)
    for i in range(2):
        for j in range(MP):
            product_sum = product_sum + vr[i, j].astype(F32)
    own_cols = pl.ds(pl.multiple_of(c * KH + m * NB, 128), NB)
    plain = product_sum * inverse + dot(low, adapter_ref[:, own_cols])
    dv = plain + bias_ref[:, own_cols] - image_targets
    dv = (dv * weight).astype(BF16)
    along = jnp.sum(dv.astype(F32) * plain, axis=1, keepdims=True)
    ss[...] = jnp.broadcast_to(along, (BT, 128)).T[:8]
    for i in range(1, 2 * MP):
        other = (me8 + i) % (2 * MP)
        send(ss, sr.at[me8], s_ss.at[i], s_rs.at[i], mp=other // 2, grp=other % 2)
    sr[me8] = ss[...]
    h_part = joined(dot(split(enc_low_t * inverse_row), dv))
    y_part = dot(low_t, dv)
    for i in range(DP):
        hys[i, 0] = h_part[i * RD : (i + 1) * RD]
        hys[i, 1] = y_part[i * RD : (i + 1) * RD]
    for i in range(1, DP):
        there = (e + i) % DP
        send(hys.at[there], hyr.at[e], hy_ss.at[i], hy_rs.at[i], dp=there)
    hyr[e] = hys[e]

    for i in range(1, 2 * MP):
        other = (here8 + 2 * MP - i) % (2 * MP)
        landed(gr.at[other // MP, other % MP], g_ss.at[i], g_rs.at[i])
    g_sum = jnp.zeros((RANK, Q), F32)
    for i in range(2):
        for j in range(MP):
            g_sum = g_sum + gr[i, j].astype(F32)
    g_pair = split(g_sum)

    def through(cols):
        part = dot(g_pair[:, :R], wq[0, :, cols])
        for i in range(1, QB):
            part = part + dot(g_pair[:, i * R : (i + 1) * R], wq[i, :, cols])
        return joined(part)

    ys[...] = through(pl.ds(oc * KH, KH))
    send(ys, yr, yp_ss, yp_rs, grp=oc)
    text_grad = text_grad + through(pl.ds(c * KH, KH))
    landed(yr, yp_ss, yp_rs)
    text_grad = text_grad + yr[...]
    for i in range(DP):
        for j in range(MP):
            yrs[i, j] = text_grad[i * RD : (i + 1) * RD, j * NB : (j + 1) * NB]
    for i in range(1, OWN):
        other = (owner + i) % OWN
        od, om = other // MP, other % MP
        send(yrs.at[od, om], yrr.at[e, m], yr_ss.at[i], yr_rs.at[i], dp=od, mp=om)
    yrr[e, m] = yrs[e, m]

    for i in range(1, 2 * MP):
        other = (me8 + 2 * MP - i) % (2 * MP)
        landed(sr.at[other], s_ss.at[i], s_rs.at[i])
    along_row = jnp.zeros((8, BT), F32)
    for i in range(2 * MP):
        along_row = along_row + sr[i]
    factor = along_row[:1] * inverse_row * inverse_row / D
    second_pair = split(enc_low_t * factor)
    for i in range(2):
        second = joined(dot(second_pair, img[:, pl.ds(i * Q, Q)])).astype(BF16)
        for j in range(UN):
            s2s[i, j] = second[j * RU : (j + 1) * RU]
    for i in range(1, DP):
        there = (e + i) % DP
        send(s2s.at[(there % 2 + c + m // 2) % 2, there // 2], s2r.at[e], s2_ss.at[i], s2_rs.at[i], dp=there)
    s2r[e] = s2s[t0, u]

    for i in range(1, DP):
        landed(hyr.at[(e + DP - i) % DP], hy_ss.at[i], hy_rs.at[i])
    hy = hyr[0]
    for i in range(1, DP):
        hy = hy + hyr[i]
    hbs[...] = hy[0]
    unit = (p * 2 + c) * MP + m
    for i in range(1, 4 * MP):
        other = (unit + i) % (4 * MP)
        send(
            hbs, hb.at[p, c, m], hb_ss.at[i], hb_rs.at[i],
            dp=2 * u + other // (2 * MP), grp=other // MP % 2, mp=other % MP,
        )
    hb[p, c, m] = hbs[...]
    for i in range(1, OWN):
        other = (owner + OWN - i) % OWN
        landed(yrr.at[other // MP, other % MP], yr_ss.at[i], yr_rs.at[i])
    y_sum = hy[1]
    for i in range(DP):
        for j in range(MP):
            y_sum = y_sum + yrr[i, j]
    yos[...] = y_sum
    DH = DP // 2
    y_core = e // DH
    y_row = e % DH
    y_there = out_llm.at[y_row, :, own_cols]
    for i in range(1, OWN):
        other = (owner + i) % OWN
        send(yos, y_there, yo_ss.at[i], yo_rs.at[y_row, m, c], dp=other // MP, mp=other % MP, grp=y_core)
    y_away = copy(yos, y_there, yo_ss.at[0], yo_rs.at[y_row, m, c], grp=oc)

    @pl.when(y_core == c)
    def _():
        out_llm[y_row, :, own_cols] = yos[...]

    @pl.when(y_core != c)
    def _():
        y_away.start()

    for i in range(1, 4 * MP):
        other = (unit + 4 * MP - i) % (4 * MP)
        landed(hb.at[other // (2 * MP), other // MP % 2, other % MP], hb_ss.at[i], hb_rs.at[i])
    h_all = jnp.concatenate(
        [
            jnp.concatenate([hb[i, j, k] for j in range(2) for k in range(MP)], axis=1)
            for i in range(2)
        ],
        axis=0,
    )
    h_pair = split(h_all)
    h_low = split(joined(dot(h_pair, adapter_ref[...], NT)))
    quarter = m * SH + half + t0 * Q
    parts = []
    for i in range(QB):
        q = quarter // R + i
        part = joined(dot(h_pair, wq[i], NT)) + joined(dot(h_low, at[q // MP, q % MP]))
        parts.append(part * gain_ref[:, pl.ds(pl.multiple_of(quarter + i * R, 128), R)])
    result = jnp.concatenate(parts, axis=1)
    for i in range(1, DP):
        landed(s2r.at[(e + DP - i) % DP], s2_ss.at[i], s2_rs.at[i])
    for i in range(DP):
        result = result - s2r[i].astype(F32)
    fo[...] = result.astype(BF16)
    UH = UN // 2
    f_core = u // UH
    f_unit = u % UH
    f_there = fin.at[f_unit, p, c]
    for i in range(1, DP):
        send(fo, f_there, fo_ss.at[i], fo_rs.at[f_unit, p, c], dp=(e + i) % DP, grp=f_core)
    f_away = copy(fo, f_there, fo_ss.at[0], fo_rs.at[f_unit, p, c], grp=oc)

    @pl.when(f_core == c)
    def _():
        fin[f_unit, p, c] = fo[...]

    @pl.when(f_core != c)
    def _():
        f_away.start()

    for i in range(DH):
        for j in range(MP):
            for k in range(2):
                other = copy(yos, out_llm.at[i, :, pl.ds(k * KH + j * NB, NB)], yo_ss.at[0], yo_rs.at[i, j, k], grp=oc)

                @pl.when(jnp.logical_not((y_core == c) & (y_row == i) & (m == j) & (c == k)))
                def _():
                    other.wait_recv()

    for i in range(UH):
        for j in range(2):
            for k in range(2):
                t_other = (j + m // 2 + k) % 2
                cols = pl.ds(pl.multiple_of(k * HC + t_other * Q, 128), Q)
                arrival = copy(fo, fin.at[i, j, k], fo_ss.at[0], fo_rs.at[i, j, k], grp=oc)

                @pl.when(jnp.logical_not((f_core == c) & (f_unit == i) & (p == j) & (c == k)))
                def _():
                    arrival.wait_recv()

                out_enc[pl.ds(i * RU, RU), cols] = fin[i, j, k].astype(F32)

    for one in pending:
        one.wait_send()
    for started, one in w_sends:

        @pl.when(started)
        def _():
            one.wait_send()

    @pl.when(y_core != c)
    def _():
        y_away.wait_send()

    @pl.when(f_core != c)
    def _():
        f_away.wait_send()


def body(
    hidden, enc_weight, enc_bias, enc_frozen, enc_adapter, text_rows, norm_gain, value_weight,
    value_bias, llm_frozen, llm_adapter, targets, dest_owner, seq_length,
):
    DP, MP = lax.axis_size("dp"), lax.axis_size("mp")
    OWN = DP * MP
    NTOK, MH = hidden.shape
    BT = NTOK * MP
    LR, D = text_rows.shape
    RANK = enc_frozen.shape[1]
    KV = llm_adapter.shape[1]
    CAP = 2 * BT // OWN
    ST = CAP + 8
    ST = ST + -ST % 16
    SH = enc_weight.shape[1]
    HC, Q = SH // 2, SH // 4
    R = value_weight.shape[0]
    UN = DP // 2
    RU, RD, RG = RANK // UN, RANK // DP, RANK // 2
    KH, NB = KV // 2, KV // (2 * MP)
    KC = 1024 if MH % 1024 == 0 else MH
    NK = MH // KC
    QB = Q // R
    RL = RANK + 8
    sizes = dict(
        DP=DP, MP=MP, NTOK=NTOK, BT=BT, CAP=CAP, ST=ST, LR=LR, D=D, MH=MH, RANK=RANK, KV=KV, NB=NB,
        SH=SH, HC=HC, Q=Q, R=R, UN=UN, RU=RU, RD=RD, RG=RG, KC=KC,
    )
    vmem = pl.BlockSpec(memory_space=pltpu.VMEM)
    hbm = pl.BlockSpec(memory_space=pl.ANY)
    V = pltpu.VMEM
    S = pltpu.SemaphoreType.DMA
    scratch = [
        V((1, D), F32), V((1, SH), F32), V((1, KV), F32),
        V((MH, HC), BF16), V((BT, MH), BF16), V((BT, HC), F32), V((BT, RANK), F32), V((BT, HC), BF16),
        V((2, BT, Q), BF16), V((BT, Q), BF16), V((QB, R, KV), BF16), V((DP, MP, RANK, R), BF16), V((LR, D), BF16),
        V((MP, 2, RANK, Q), BF16), V((2, MP, RANK, Q), BF16), V((DP, MP, ST, NB), BF16), V((DP, MP, ST, NB), BF16),
        V((RL, BT), F32), V((MP, RL, BT), F32),
        V((2, BT, KH), F32), V((2, BT, KH), BF16), V((2, BT, KH), BF16),
        V((2, MP, BT, NB), BF16), V((2, MP, BT, NB), BF16),
        V((RL, BT), F32),
        V((RANK, KH), F32), V((RANK, KH), F32), V((DP, MP, RD, NB), F32), V((DP, MP, RD, NB), F32),
        V((8, BT), F32), V((2 * MP, 8, BT), F32), V((DP, 2, RD, NB), F32), V((DP, 2, RD, NB), F32),
        V((RD, NB), F32), V((2, 2, MP, RD, NB), F32), V((RD, NB), F32),
        V((2, UN, RU, Q), BF16), V((DP, RU, Q), BF16), V((RU, Q), BF16), V((UN // 2, 2, 2, RU, Q), BF16),
        S((NK,)), S(()), S(()), S((NK, MP)), S((NK, MP)), S((NK, MP)), S((NK, MP)),
        S(((UN + 1) // 2,)), S((QB,)), S(()), S(()), S((DP,)), S((DP,)), S((MP,)), S((MP,)),
        S(()), S(()), S((OWN,)), S((OWN,)), S(()), S(()), S((2 * MP,)), S((2 * MP,)), S((2 * MP,)), S((2 * MP,)),
        S((2,)), S((2,)), S((2 * MP,)), S((2 * MP,)),
        S(()), S(()), S((OWN,)), S((OWN,)), S((2 * MP,)), S((2 * MP,)), S((DP,)), S((DP,)),
        S((4 * MP,)), S((4 * MP,)), S((OWN,)), S((DP // 2, MP, 2)),
        S((DP,)), S((DP,)), S((DP,)), S((UN // 2, 2, 2)),
    ]
    grad_enc, grad_llm = pl.pallas_call(
        functools.partial(kernel, sizes),
        out_shape=(
            jax.ShapeDtypeStruct((RG, SH), F32),
            jax.ShapeDtypeStruct((DP // 2, RD, KV), F32),
        ),
        in_specs=[hbm, hbm, vmem, vmem, vmem, hbm, vmem, hbm, vmem, vmem, vmem, vmem, vmem, vmem],
        out_specs=(vmem, vmem),
        scratch_shapes=scratch,
        compiler_params=pltpu.CompilerParams(
            collective_id=0, has_side_effects=True, vmem_limit_bytes=60 * 1024 * 1024
        ),
    )(
        hidden, enc_weight, enc_bias.reshape(-1, 128), enc_frozen.T, enc_adapter, text_rows,
        norm_gain.reshape(-1, 128), value_weight, value_bias.reshape(-1, 128), llm_frozen.T, llm_adapter,
        targets, dest_owner.T, seq_length.reshape(1, 1),
    )
    return grad_enc, grad_llm.reshape(RG, KV)


def solution(mesh):
    return jax.shard_map(
        body,
        mesh=mesh,
        in_specs=(
            P(("dp", "mp"), None), P(None, "mp"), P("mp"), P(), P(None, "mp"), P(("dp", "mp"), None), P(),
            P(("dp", "mp"), None), P(), P(("dp", "mp"), None), P(), P(("dp", "mp"), None), P(), P(("dp", "mp")),
        ),
        out_specs=(P("grp", "mp"), P("grp", None)),
        check_vma=False,
    )
```

```python
import functools

import jax
import jax.numpy as jnp
from jax import lax
from jax.experimental import pallas as pl
from jax.experimental.pallas import tpu as pltpu
from jax.sharding import PartitionSpec as P

epsilon = 1e-06
TG_AT = 0
W_AT = 1
NORM_AT = 1
F32 = jnp.float32
BF16 = jnp.bfloat16
MESH = pl.DeviceIdType.MESH
NN = (((1,), (0,)), ((), ()))
NT = (((1,), (1,)), ((), ()))


def dot(a, b, dims=NN):
    return lax.dot_general(a, b, dims, preferred_element_type=F32)


def split(x):
    high = x.astype(BF16)
    rest = (x - high.astype(F32)).astype(BF16)
    return jnp.concatenate([high, rest], axis=0)


def joined(x):
    half = x.shape[0] // 2
    return x[:half] + x[half:]


def eye(n):
    return (
        lax.broadcasted_iota(jnp.int32, (n, n), 0) == lax.broadcasted_iota(jnp.int32, (n, n), 1)
    ).astype(BF16)


def kernel(
    sizes,
    hidden, enc_weight, enc_bias_in, enc_frozen, enc_adapter, text_rows, gain_in, value_weight,
    bias_in, llm_frozen, adapter_ref, targets, dest, seq_length,
    out_enc, out_llm,
    gain_ref, enc_bias, bias_ref, ebuf, hid, acc, acc_low, img, xq, xr, wq, at, txt, gs, gr, tgs, tgr, los, lor,
    vown, vps, vpr, vs, vr, lop, ys, yr, yrs, yrr, ss, sr, hys, hyr, hbs, hb, yos, s2s, s2r, fo, fin,
    e_sem, t_sem, own_sem, h_ss, h_rs, hf_ss, hf_rs, w_ss, w_rs, lp_ss, lp_rs, a1_ss, a1_rs, a2_ss, a2_rs,
    a3_ss, a3_rs, tg_ss, tg_rs, x_ss, x_rs, lo_ss, lo_rs, g_ss, g_rs, vp_ss, vp_rs, v_ss, v_rs,
    yp_ss, yp_rs, yr_ss, yr_rs, s_ss, s_rs, hy_ss, hy_rs, hb_ss, hb_rs, yo_ss, yo_rs,
    s2_ss, s2_rs, fo_ss, fo_rs,
):
    z = sizes
    DP, MP = z["DP"], z["MP"]
    NTOK, BT, CAP, ST, LR = z["NTOK"], z["BT"], z["CAP"], z["ST"], z["LR"]
    D, MH, RANK, KV, NB = z["D"], z["MH"], z["RANK"], z["KV"], z["NB"]
    SH, HC, Q, R, UN, RU, RD, RG, KC = (z[k] for k in ("SH", "HC", "Q", "R", "UN", "RU", "RD", "RG", "KC"))
    KH = KV // 2
    NK = MH // KC
    QB = Q // R
    OWN = DP * MP
    c = lax.axis_index("grp")
    e = lax.axis_index("dp")
    m = lax.axis_index("mp")
    p, u = e % 2, e // 2
    oc = 1 - c
    t0 = (p + m // 2 + c) % 2
    owner = e * MP + m
    pending = []

    def copy(src, dst, ssem, rsem, dp=None, mp=None, grp=None):
        device = {"grp": c if grp is None else grp, "dp": e if dp is None else dp, "mp": m if mp is None else mp}
        return pltpu.make_async_remote_copy(
            src_ref=src, dst_ref=dst, send_sem=ssem, recv_sem=rsem, device_id=device, device_id_type=MESH
        )

    def send(*args, **kw):
        made = copy(*args, **kw)
        made.start()
        pending.append(made)

    def landed(dst, ssem, rsem):
        copy(dst, dst, ssem, rsem, grp=oc).wait_recv()

    barrier = pltpu.get_barrier_semaphore()
    devices = 2 * OWN
    place = (c * DP + e) * MP + m

    def greet(i, carry):
        other = (place + i) % devices
        device = {"grp": other // OWN, "dp": other // MP % DP, "mp": other % MP}
        pl.semaphore_signal(barrier, inc=1, device_id=device, device_id_type=MESH)
        return carry

    lax.fori_loop(1, devices, greet, 0)

    half = c * HC
    loads = []
    for k in range(NK):
        one = pltpu.make_async_copy(
            enc_weight.at[pl.ds(k * KC, KC), pl.ds(half, HC)], ebuf.at[pl.ds(k * KC, KC), :], e_sem.at[k]
        )
        loads.append(one)
    text_load = pltpu.make_async_copy(text_rows, txt, t_sem)
    own_load = pltpu.make_async_copy(hidden, hid.at[pl.ds(m * NTOK, NTOK), :], own_sem)
    own_load.start()
    text_load.start()
    for one in loads:
        one.start()

    RH = RANK // 2
    low_half = c * RH
    at[e, m, pl.ds(low_half, RH), :] = llm_frozen[pl.ds(pl.multiple_of(low_half, 16), RH), :]
    for packed, row in ((gain_in, gain_ref), (enc_bias_in, enc_bias), (bias_in, bias_ref)):
        wide = packed[...].astype(F32)
        for i in range(wide.shape[0]):
            row[:, i * 128 : (i + 1) * 128] = wide[i : i + 1]
    rows = CAP * DP
    order_i = lax.broadcasted_iota(jnp.int32, (rows, rows), 0)
    order_j = lax.broadcasted_iota(jnp.int32, (rows, rows), 1)
    order = (order_j == order_i % CAP * DP + order_i // CAP).astype(BF16)
    sorted_targets = dot(order, targets[pl.ds(0, rows), pl.ds(c * KH, KH)]).astype(BF16)
    length = seq_length[...].astype(F32)
    for i in range(DP):
        for j in range(MP):
            block = sorted_targets[i * CAP : (i + 1) * CAP, j * NB : (j + 1) * NB]
            tail = jnp.broadcast_to(length, (ST - CAP, NB)).astype(BF16)
            tgs[i, j] = jnp.concatenate([block, tail], axis=0)

    pl.semaphore_wait(barrier, devices - 1)

    w_sends = []

    def send_weights():
        w_row = owner * R
        w_m = w_row // SH
        w_t = w_row % SH // Q
        w_slot = w_row % Q // R
        w_core = w_t // 2
        w_par = (w_t % 2 + w_t // 2 + w_m // 2) % 2
        for i in range((UN + 1) // 2):
            w_u = 2 * i + c
            there = 2 * w_u + w_par
            self_case = (there == e) & (w_m == m) & (w_core == c)
            live = w_u < UN
            away = copy(value_weight, wq.at[w_slot], w_ss.at[i], w_rs.at[w_slot], dp=there, mp=w_m, grp=w_core)
            near = pltpu.make_async_copy(value_weight, wq.at[w_slot], w_rs.at[w_slot])
            w_sends.append((live & jnp.logical_not(self_case), away))

            @pl.when(live & jnp.logical_not(self_case))
            def _():
                away.start()

            @pl.when(live & self_case)
            def _():
                near.start()

    for i in range(1, DP):
        mine = at.at[e, m, pl.ds(low_half, RH), :]
        send(mine, mine, a1_ss.at[i], a1_rs.at[i], dp=(e + i) % DP)
    NH = NTOK // 2
    hid_rows = pl.ds(m * NTOK + c * NH, NH)
    for k in range(NK):
        cols = pl.ds(k * KC, KC)
        for i in range(1, MP):
            send(hidden.at[pl.ds(c * NH, NH), cols], hid.at[hid_rows, cols], h_ss.at[k, i], h_rs.at[k, i], mp=(m + i) % MP)
    tgr[e, m] = tgs[e, m]

    def norm_text():
        text_load.wait()
        TR = 16
        CW = min(D, 1024)

        def text_norm(i, carry):
            r = pl.ds(i * TR, TR)
            total = jnp.zeros((TR, 128), F32)
            for k in range(D // CW):
                part = txt[r, pl.ds(k * CW, CW)].astype(F32)
                part = part * part
                for n in range(CW // 128):
                    total = total + part[:, n * 128 : (n + 1) * 128]
            inverse = lax.rsqrt(jnp.sum(total, axis=1, keepdims=True) / D + epsilon)
            for k in range(D // CW):
                cols = pl.ds(k * CW, CW)
                txt[r, cols] = (txt[r, cols].astype(F32) * inverse * gain_ref[:, cols]).astype(BF16)
            return carry

        lax.fori_loop(0, LR // TR, text_norm, 0)

    if NORM_AT == 0:
        norm_text()

    for i in range(1, DP):
        there = at.at[(e + DP - i) % DP, m, pl.ds(low_half, RH), :]
        landed(there, a1_ss.at[i], a1_rs.at[i])
    if W_AT == 0:
        send_weights()
    for i in range(1, MP):
        mine = at.at[:, m, pl.ds(low_half, RH), :]
        send(mine, mine, a2_ss.at[i], a2_rs.at[i], mp=(m + i) % MP)

    if W_AT == 1:
        send_weights()

    if NORM_AT == 1:
        norm_text()

    own_load.wait()
    TN = min(HC, 256)
    for k in range(NK):
        cols = pl.ds(k * KC, KC)
        for i in range(1, MP):
            peer = (m + MP - i) % MP
            there = hid.at[pl.ds(peer * NTOK + c * NH, NH), cols]
            landed(there, h_ss.at[k, i], h_rs.at[k, i])
            send(there, there, hf_ss.at[k, i], hf_rs.at[k, i], grp=oc)
        loads[k].wait()
        for i in range(1, MP):
            peer = (m + MP - i) % MP
            there = hid.at[pl.ds(peer * NTOK + oc * NH, NH), cols]
            landed(there, hf_ss.at[k, i], hf_rs.at[k, i])

        def product(n, carry):
            part = dot(hid[:, cols], ebuf[cols, pl.ds(n * TN, TN)])
            if k == 0:
                acc[:, pl.ds(n * TN, TN)] = part
            else:
                acc[:, pl.ds(n * TN, TN)] += part
            return carry

        lax.fori_loop(0, HC // TN, product, 0)
        low_part = dot(hid[:, cols], enc_frozen[:, cols], NT)
        if k == 0:
            acc_low[...] = low_part
        else:
            acc_low[...] += low_part
    enc_low = acc_low[...].astype(BF16)
    enc_low_t = dot(eye(RANK), enc_low, NT)
    squares = jnp.zeros((BT, 128), F32)
    for n in range(HC // TN):
        cols = pl.ds(n * TN, TN)
        shifted = pl.ds(half + n * TN, TN)
        merged = acc[:, cols] + enc_bias[:, shifted] + dot(enc_low, enc_adapter[:, shifted])
        merged = merged.astype(BF16)
        img[:, cols] = merged
        wide = merged.astype(F32)
        square = wide * wide
        for i in range(TN // 128):
            squares = squares + square[:, i * 128 : (i + 1) * 128]
        scaled = (wide * gain_ref[:, pl.ds(m * SH + half + n * TN, TN)]).astype(BF16)
        xq[n * TN // Q, :, n * TN % Q : n * TN % Q + TN] = scaled
    pair = e + 1 - 2 * p
    send(xq.at[1 - t0], xr, x_ss, x_rs, dp=pair)
    if TG_AT == 0:
        for i in range(1, OWN):
            other = (owner + i) % OWN
            od, om = other // MP, other % MP
            send(tgs.at[od, om], tgr.at[e, m], tg_ss.at[i], tg_rs.at[i], dp=od, mp=om)

    for i in range(1, MP):
        there = at.at[:, (m + MP - i) % MP, pl.ds(low_half, RH), :]
        landed(there, a2_ss.at[i], a2_rs.at[i])
    mine = at.at[:, :, pl.ds(low_half, RH), :]
    send(mine, mine, a3_ss, a3_rs, grp=oc)
    landed(at.at[:, :, pl.ds(oc * RH, RH), :], a3_ss, a3_rs)

    first = (m * SH + half) // R
    low_part = jnp.zeros((RANK, BT), F32)
    for i in range(HC // R):
        q = first + i
        x = xq[i * R // Q, :, i * R % Q : i * R % Q + R]
        low_part = low_part + dot(at[q // MP, q % MP], x, NT)
    total = jnp.broadcast_to(jnp.sum(squares, axis=1, keepdims=True), (BT, 128))
    los[...] = jnp.concatenate([low_part, total.T[:8]], axis=0)
    me8 = m * 2 + c
    send(los, lop, lp_ss, lp_rs, grp=oc)
    landed(lop, lp_ss, lp_rs)
    lor[m] = los[...] + lop[...]
    for i in range(1, MP):
        send(lor.at[m], lor.at[m], lo_ss.at[i], lo_rs.at[i], mp=(m + i) % MP)
    if TG_AT == 1:
        for i in range(1, OWN):
            other = (owner + i) % OWN
            od, om = other // MP, other % MP
            send(tgs.at[od, om], tgr.at[e, m], tg_ss.at[i], tg_rs.at[i], dp=od, mp=om)

    def text_low(q, carry):
        part = txt[:, pl.ds(pl.multiple_of(q * R, 128), R)]
        return carry + dot(part, at[q // MP, q % MP], NT)

    text_low_n = lax.fori_loop(0, OWN, text_low, jnp.zeros((LR, RANK), F32))
    text_low_b = text_low_n.astype(BF16)
    text_low_t = jnp.concatenate([text_low_b.astype(F32), jnp.zeros((LR, 128 - RANK), F32)], axis=1).T[:RANK]
    place_row = lax.broadcasted_iota(jnp.int32, (8, LR), 1)
    count = jnp.zeros((8, LR), F32)
    for i in range(DP):
        named = (dest[:, i * BT : (i + 1) * BT] == owner).astype(F32)
        named = jnp.sum(named, axis=1, keepdims=True)
        count = jnp.where(place_row % DP == i, jnp.broadcast_to(named, (8, LR)), count)
    replaced = (place_row < CAP * DP) & ((place_row // DP).astype(F32) < count)
    live = (place_row.astype(F32) < jnp.broadcast_to(length, (8, LR))) & jnp.logical_not(replaced)
    live = jnp.where(live, 1.0, 0.0)[:1]
    text_low_m = (text_low_t * live).astype(BF16)
    scale = 1.0 / length
    here8 = p * MP + m
    for j in range(MP):
        for i in range(2):
            col = pl.multiple_of(j * SH + half + i * Q, 128)
            gs[j, i] = (dot(text_low_m, txt[:, pl.ds(col, Q)]) * scale).astype(BF16)
    for i in range(1, 2 * MP):
        other = (here8 + i) % (2 * MP)
        gp, gm = other // MP, other % MP
        send(gs.at[gm, (gp + gm // 2 + c) % 2], gr.at[p, m], g_ss.at[i], g_rs.at[i], dp=2 * u + gp, mp=gm)
    gr[p, m] = gs[m, t0]
    text_y = dot(text_low_b, adapter_ref[:, pl.ds(c * KH, KH)])
    text_y = text_y + bias_ref[:, pl.ds(c * KH, KH)] - targets[:, pl.ds(c * KH, KH)].astype(F32)
    high = text_y.astype(BF16)
    rest = (text_y - high.astype(F32)).astype(BF16)
    text_grad = (dot(text_low_m, high) + dot(text_low_m, rest)) * scale

    if TG_AT == 2:
        for i in range(1, OWN):
            other = (owner + i) % OWN
            od, om = other // MP, other % MP
            send(tgs.at[od, om], tgr.at[e, m], tg_ss.at[i], tg_rs.at[i], dp=od, mp=om)

    for i in range(QB):
        landed(wq.at[i], w_ss.at[0], w_rs.at[i])

    def values_of(x, where, first_col):
        for n in range(KH // TN):
            cols = pl.ds(pl.multiple_of(first_col + n * TN, 128), TN)
            part = dot(x[:, :R], wq[0, :, cols])
            for i in range(1, QB):
                part = part + dot(x[:, i * R : (i + 1) * R], wq[i, :, cols])
            where[:, n * TN : (n + 1) * TN] = part.astype(where.dtype)

    values_of(xq[t0], vps.at[p], oc * KH)
    send(vps.at[p], vpr.at[p], vp_ss.at[0], vp_rs.at[0], grp=oc)
    landed(xr, x_ss, x_rs)
    values_of(xr[...], vps.at[1 - p], oc * KH)
    send(vps.at[1 - p], vpr.at[1 - p], vp_ss.at[1], vp_rs.at[1], grp=oc)
    values_of(xq[t0], vown.at[p], c * KH)
    values_of(xr[...], vown.at[1 - p], c * KH)
    landed(vpr.at[p], vp_ss.at[0], vp_rs.at[0])
    landed(vpr.at[1 - p], vp_ss.at[1], vp_rs.at[1])
    for i in range(2):
        both = (vown[i] + vpr[i]).astype(BF16)
        for j in range(MP):
            vs[i, j] = both[:, j * NB : (j + 1) * NB]
    for i in range(1, 2 * MP):
        other = (here8 + i) % (2 * MP)
        gp, gm = other // MP, other % MP
        send(vs.at[gp, gm], vr.at[p, m], v_ss.at[i], v_rs.at[i], dp=2 * u + gp, mp=gm)
    vr[p, m] = vs[p, m]

    for i in range(1, OWN):
        other = (owner + OWN - i) % OWN
        landed(tgr.at[other // MP, other % MP], tg_ss.at[i], tg_rs.at[i])
    block_dest = dest[:, pl.ds(pl.multiple_of(e * BT, 128), BT)].astype(F32)
    block_dest = jnp.broadcast_to(block_dest, (128, BT)).T
    marks = block_dest == lax.broadcasted_iota(jnp.int32, (BT, 128), 1).astype(F32)
    before = lax.broadcasted_iota(jnp.int32, (BT, BT), 0) > lax.broadcasted_iota(jnp.int32, (BT, BT), 1)
    counted = dot(before.astype(BF16), marks.astype(BF16))
    slot = jnp.sum(jnp.where(marks, counted, 0.0), axis=1, keepdims=True)
    base = block_dest[:, :1] * ST
    table_rows = lax.broadcasted_iota(jnp.int32, (BT, OWN * ST), 1).astype(F32)
    table = tgr[...].reshape(OWN * ST, NB)
    image_targets = dot((table_rows == base + slot).astype(BF16), table)
    image_length = dot((table_rows == base + CAP).astype(BF16), table)
    position = slot * DP + e.astype(F32)
    weight = jnp.where(position < image_length, 1.0 / image_length, 0.0)

    gathered = jnp.zeros((RANK + 8, BT), F32)
    for i in range(1, MP):
        landed(lor.at[(m + MP - i) % MP], lo_ss.at[i], lo_rs.at[i])
    for i in range(MP):
        gathered = gathered + lor[i]
    inverse_row = lax.rsqrt(gathered[RANK : RANK + 1] / D + epsilon)
    low_t = (gathered[:RANK] * inverse_row).astype(BF16)
    turned = jnp.concatenate(
        [low_t.astype(F32), jnp.broadcast_to(inverse_row, (128 - RANK, BT))], axis=0
    ).T
    low = turned[:, :RANK].astype(BF16)
    inverse = turned[:, RANK : RANK + 1]

    for i in range(1, 2 * MP):
        other = (here8 + 2 * MP - i) % (2 * MP)
        landed(vr.at[other // MP, other % MP], v_ss.at[i], v_rs.at[i])
    product_sum = jnp.zeros((BT, NB), F32)
    for i in range(2):
        for j in range(MP):
            product_sum = product_sum + vr[i, j].astype(F32)
    own_cols = pl.ds(pl.multiple_of(c * KH + m * NB, 128), NB)
    plain = product_sum * inverse + dot(low, adapter_ref[:, own_cols])
    dv = plain + bias_ref[:, own_cols] - image_targets
    dv = (dv * weight).astype(BF16)
    along = jnp.sum(dv.astype(F32) * plain, axis=1, keepdims=True)
    ss[...] = jnp.broadcast_to(along, (BT, 128)).T[:8]
    for i in range(1, 2 * MP):
        other = (me8 + i) % (2 * MP)
        send(ss, sr.at[me8], s_ss.at[i], s_rs.at[i], mp=other // 2, grp=other % 2)
    sr[me8] = ss[...]
    h_part = joined(dot(split(enc_low_t * inverse_row), dv))
    y_part = dot(low_t, dv)
    for i in range(DP):
        hys[i, 0] = h_part[i * RD : (i + 1) * RD]
        hys[i, 1] = y_part[i * RD : (i + 1) * RD]
    for i in range(1, DP):
        there = (e + i) % DP
        send(hys.at[there], hyr.at[e], hy_ss.at[i], hy_rs.at[i], dp=there)
    hyr[e] = hys[e]

    for i in range(1, 2 * MP):
        other = (here8 + 2 * MP - i) % (2 * MP)
        landed(gr.at[other // MP, other % MP], g_ss.at[i], g_rs.at[i])
    g_sum = jnp.zeros((RANK, Q), F32)
    for i in range(2):
        for j in range(MP):
            g_sum = g_sum + gr[i, j].astype(F32)
    g_pair = split(g_sum)

    def through(cols):
        part = dot(g_pair[:, :R], wq[0, :, cols])
        for i in range(1, QB):
            part = part + dot(g_pair[:, i * R : (i + 1) * R], wq[i, :, cols])
        return joined(part)

    ys[...] = through(pl.ds(oc * KH, KH))
    send(ys, yr, yp_ss, yp_rs, grp=oc)
    text_grad = text_grad + through(pl.ds(c * KH, KH))
    landed(yr, yp_ss, yp_rs)
    text_grad = text_grad + yr[...]
    for i in range(DP):
        for j in range(MP):
            yrs[i, j] = text_grad[i * RD : (i + 1) * RD, j * NB : (j + 1) * NB]
    for i in range(1, OWN):
        other = (owner + i) % OWN
        od, om = other // MP, other % MP
        send(yrs.at[od, om], yrr.at[e, m], yr_ss.at[i], yr_rs.at[i], dp=od, mp=om)
    yrr[e, m] = yrs[e, m]

    for i in range(1, 2 * MP):
        other = (me8 + 2 * MP - i) % (2 * MP)
        landed(sr.at[other], s_ss.at[i], s_rs.at[i])
    along_row = jnp.zeros((8, BT), F32)
    for i in range(2 * MP):
        along_row = along_row + sr[i]
    factor = along_row[:1] * inverse_row * inverse_row / D
    second_pair = split(enc_low_t * factor)
    for i in range(2):
        second = joined(dot(second_pair, img[:, pl.ds(i * Q, Q)])).astype(BF16)
        for j in range(UN):
            s2s[i, j] = second[j * RU : (j + 1) * RU]
    for i in range(1, DP):
        there = (e + i) % DP
        send(s2s.at[(there % 2 + c + m // 2) % 2, there // 2], s2r.at[e], s2_ss.at[i], s2_rs.at[i], dp=there)
    s2r[e] = s2s[t0, u]

    for i in range(1, DP):
        landed(hyr.at[(e + DP - i) % DP], hy_ss.at[i], hy_rs.at[i])
    hy = hyr[0]
    for i in range(1, DP):
        hy = hy + hyr[i]
    hbs[...] = hy[0]
    unit = (p * 2 + c) * MP + m
    for i in range(1, 4 * MP):
        other = (unit + i) % (4 * MP)
        send(
            hbs, hb.at[p, c, m], hb_ss.at[i], hb_rs.at[i],
            dp=2 * u + other // (2 * MP), grp=other // MP % 2, mp=other % MP,
        )
    hb[p, c, m] = hbs[...]
    for i in range(1, OWN):
        other = (owner + OWN - i) % OWN
        landed(yrr.at[other // MP, other % MP], yr_ss.at[i], yr_rs.at[i])
    y_sum = hy[1]
    for i in range(DP):
        for j in range(MP):
            y_sum = y_sum + yrr[i, j]
    yos[...] = y_sum
    DH = DP // 2
    y_core = e // DH
    y_row = e % DH
    y_there = out_llm.at[y_row, :, own_cols]
    for i in range(1, OWN):
        other = (owner + i) % OWN
        send(yos, y_there, yo_ss.at[i], yo_rs.at[y_row, m, c], dp=other // MP, mp=other % MP, grp=y_core)
    y_away = copy(yos, y_there, yo_ss.at[0], yo_rs.at[y_row, m, c], grp=oc)

    @pl.when(y_core == c)
    def _():
        out_llm[y_row, :, own_cols] = yos[...]

    @pl.when(y_core != c)
    def _():
        y_away.start()

    for i in range(1, 4 * MP):
        other = (unit + 4 * MP - i) % (4 * MP)
        landed(hb.at[other // (2 * MP), other // MP % 2, other % MP], hb_ss.at[i], hb_rs.at[i])
    h_all = jnp.concatenate(
        [
            jnp.concatenate([hb[i, j, k] for j in range(2) for k in range(MP)], axis=1)
            for i in range(2)
        ],
        axis=0,
    )
    h_pair = split(h_all)
    h_low = split(joined(dot(h_pair, adapter_ref[...], NT)))
    quarter = m * SH + half + t0 * Q
    parts = []
    for i in range(QB):
        q = quarter // R + i
        part = joined(dot(h_pair, wq[i], NT)) + joined(dot(h_low, at[q // MP, q % MP]))
        parts.append(part * gain_ref[:, pl.ds(pl.multiple_of(quarter + i * R, 128), R)])
    result = jnp.concatenate(parts, axis=1)
    for i in range(1, DP):
        landed(s2r.at[(e + DP - i) % DP], s2_ss.at[i], s2_rs.at[i])
    for i in range(DP):
        result = result - s2r[i].astype(F32)
    fo[...] = result.astype(BF16)
    UH = UN // 2
    f_core = u // UH
    f_unit = u % UH
    f_there = fin.at[f_unit, p, c]
    for i in range(1, DP):
        send(fo, f_there, fo_ss.at[i], fo_rs.at[f_unit, p, c], dp=(e + i) % DP, grp=f_core)
    f_away = copy(fo, f_there, fo_ss.at[0], fo_rs.at[f_unit, p, c], grp=oc)

    @pl.when(f_core == c)
    def _():
        fin[f_unit, p, c] = fo[...]

    @pl.when(f_core != c)
    def _():
        f_away.start()

    for i in range(DH):
        for j in range(MP):
            for k in range(2):
                other = copy(yos, out_llm.at[i, :, pl.ds(k * KH + j * NB, NB)], yo_ss.at[0], yo_rs.at[i, j, k], grp=oc)

                @pl.when(jnp.logical_not((y_core == c) & (y_row == i) & (m == j) & (c == k)))
                def _():
                    other.wait_recv()

    for i in range(UH):
        for j in range(2):
            for k in range(2):
                t_other = (j + m // 2 + k) % 2
                cols = pl.ds(pl.multiple_of(k * HC + t_other * Q, 128), Q)
                arrival = copy(fo, fin.at[i, j, k], fo_ss.at[0], fo_rs.at[i, j, k], grp=oc)

                @pl.when(jnp.logical_not((f_core == c) & (f_unit == i) & (p == j) & (c == k)))
                def _():
                    arrival.wait_recv()

                out_enc[pl.ds(i * RU, RU), cols] = fin[i, j, k].astype(F32)

    for one in pending:
        one.wait_send()
    for started, one in w_sends:

        @pl.when(started)
        def _():
            one.wait_send()

    @pl.when(y_core != c)
    def _():
        y_away.wait_send()

    @pl.when(f_core != c)
    def _():
        f_away.wait_send()


def body(
    hidden, enc_weight, enc_bias, enc_frozen, enc_adapter, text_rows, norm_gain, value_weight,
    value_bias, llm_frozen, llm_adapter, targets, dest_owner, seq_length,
):
    DP, MP = lax.axis_size("dp"), lax.axis_size("mp")
    OWN = DP * MP
    NTOK, MH = hidden.shape
    BT = NTOK * MP
    LR, D = text_rows.shape
    RANK = enc_frozen.shape[1]
    KV = llm_adapter.shape[1]
    CAP = 2 * BT // OWN
    ST = CAP + 8
    ST = ST + -ST % 16
    SH = enc_weight.shape[1]
    HC, Q = SH // 2, SH // 4
    R = value_weight.shape[0]
    UN = DP // 2
    RU, RD, RG = RANK // UN, RANK // DP, RANK // 2
    KH, NB = KV // 2, KV // (2 * MP)
    KC = 1024 if MH % 1024 == 0 else MH
    NK = MH // KC
    QB = Q // R
    RL = RANK + 8
    sizes = dict(
        DP=DP, MP=MP, NTOK=NTOK, BT=BT, CAP=CAP, ST=ST, LR=LR, D=D, MH=MH, RANK=RANK, KV=KV, NB=NB,
        SH=SH, HC=HC, Q=Q, R=R, UN=UN, RU=RU, RD=RD, RG=RG, KC=KC,
    )
    vmem = pl.BlockSpec(memory_space=pltpu.VMEM)
    hbm = pl.BlockSpec(memory_space=pl.ANY)
    V = pltpu.VMEM
    S = pltpu.SemaphoreType.DMA
    scratch = [
        V((1, D), F32), V((1, SH), F32), V((1, KV), F32),
        V((MH, HC), BF16), V((BT, MH), BF16), V((BT, HC), F32), V((BT, RANK), F32), V((BT, HC), BF16),
        V((2, BT, Q), BF16), V((BT, Q), BF16), V((QB, R, KV), BF16), V((DP, MP, RANK, R), BF16), V((LR, D), BF16),
        V((MP, 2, RANK, Q), BF16), V((2, MP, RANK, Q), BF16), V((DP, MP, ST, NB), BF16), V((DP, MP, ST, NB), BF16),
        V((RL, BT), F32), V((MP, RL, BT), F32),
        V((2, BT, KH), F32), V((2, BT, KH), F32), V((2, BT, KH), F32),
        V((2, MP, BT, NB), BF16), V((2, MP, BT, NB), BF16),
        V((RL, BT), F32),
        V((RANK, KH), F32), V((RANK, KH), F32), V((DP, MP, RD, NB), F32), V((DP, MP, RD, NB), F32),
        V((8, BT), F32), V((2 * MP, 8, BT), F32), V((DP, 2, RD, NB), F32), V((DP, 2, RD, NB), F32),
        V((RD, NB), F32), V((2, 2, MP, RD, NB), F32), V((RD, NB), F32),
        V((2, UN, RU, Q), BF16), V((DP, RU, Q), BF16), V((RU, Q), BF16), V((UN // 2, 2, 2, RU, Q), BF16),
        S((NK,)), S(()), S(()), S((NK, MP)), S((NK, MP)), S((NK, MP)), S((NK, MP)),
        S(((UN + 1) // 2,)), S((QB,)), S(()), S(()), S((DP,)), S((DP,)), S((MP,)), S((MP,)),
        S(()), S(()), S((OWN,)), S((OWN,)), S(()), S(()), S((2 * MP,)), S((2 * MP,)), S((2 * MP,)), S((2 * MP,)),
        S((2,)), S((2,)), S((2 * MP,)), S((2 * MP,)),
        S(()), S(()), S((OWN,)), S((OWN,)), S((2 * MP,)), S((2 * MP,)), S((DP,)), S((DP,)),
        S((4 * MP,)), S((4 * MP,)), S((OWN,)), S((DP // 2, MP, 2)),
        S((DP,)), S((DP,)), S((DP,)), S((UN // 2, 2, 2)),
    ]
    grad_enc, grad_llm = pl.pallas_call(
        functools.partial(kernel, sizes),
        out_shape=(
            jax.ShapeDtypeStruct((RG, SH), F32),
            jax.ShapeDtypeStruct((DP // 2, RD, KV), F32),
        ),
        in_specs=[hbm, hbm, vmem, vmem, vmem, hbm, vmem, hbm, vmem, vmem, vmem, vmem, vmem, vmem],
        out_specs=(vmem, vmem),
        scratch_shapes=scratch,
        compiler_params=pltpu.CompilerParams(
            collective_id=0, has_side_effects=True, vmem_limit_bytes=60 * 1024 * 1024
        ),
    )(
        hidden, enc_weight, enc_bias.reshape(-1, 128), enc_frozen.T, enc_adapter, text_rows,
        norm_gain.reshape(-1, 128), value_weight, value_bias.reshape(-1, 128), llm_frozen.T, llm_adapter,
        targets, dest_owner.T, seq_length.reshape(1, 1),
    )
    return grad_enc, grad_llm.reshape(RG, KV)


def solution(mesh):
    return jax.shard_map(
        body,
        mesh=mesh,
        in_specs=(
            P(("dp", "mp"), None), P(None, "mp"), P("mp"), P(), P(None, "mp"), P(("dp", "mp"), None), P(),
            P(("dp", "mp"), None), P(), P(("dp", "mp"), None), P(), P(("dp", "mp"), None), P(), P(("dp", "mp")),
        ),
        out_specs=(P("grp", "mp"), P("grp", None)),
        check_vma=False,
    )
```

```python
import functools

import jax
import jax.numpy as jnp
from jax import lax
from jax.experimental import pallas as pl
from jax.experimental.pallas import tpu as pltpu
from jax.sharding import PartitionSpec as P

epsilon = 1e-06
TG_AT = 0
W_AT = 1
NORM_AT = 1
F32 = jnp.float32
BF16 = jnp.bfloat16
MESH = pl.DeviceIdType.MESH
NN = (((1,), (0,)), ((), ()))
NT = (((1,), (1,)), ((), ()))


def dot(a, b, dims=NN):
    return lax.dot_general(a, b, dims, preferred_element_type=F32)


def split(x):
    high = x.astype(BF16)
    rest = (x - high.astype(F32)).astype(BF16)
    return jnp.concatenate([high, rest], axis=0)


def joined(x):
    half = x.shape[0] // 2
    return x[:half] + x[half:]


def eye(n):
    return (
        lax.broadcasted_iota(jnp.int32, (n, n), 0) == lax.broadcasted_iota(jnp.int32, (n, n), 1)
    ).astype(BF16)


def kernel(
    sizes,
    hidden, enc_weight, enc_bias_in, enc_frozen, enc_adapter, text_rows, gain_in, value_weight,
    bias_in, llm_frozen, adapter_ref, targets, dest, seq_length,
    out_enc, out_llm,
    gain_ref, enc_bias, bias_ref, ebuf, hid, acc, acc_low, img, xq, xr, wq, at, txt, gs, gr, tgs, tgr, los, lor,
    vown, vps, vpr, vs, vr, lop, ys, yr, yrs, yrr, ss, sr, hys, hyr, hbs, hb, yos, s2s, s2r, fo, fin,
    e_sem, t_sem, own_sem, h_ss, h_rs, hf_ss, hf_rs, w_ss, w_rs, lp_ss, lp_rs, a1_ss, a1_rs, a2_ss, a2_rs,
    a3_ss, a3_rs, tg_ss, tg_rs, x_ss, x_rs, lo_ss, lo_rs, g_ss, g_rs, vp_ss, vp_rs, v_ss, v_rs,
    yp_ss, yp_rs, yr_ss, yr_rs, s_ss, s_rs, hy_ss, hy_rs, hb_ss, hb_rs, yo_ss, yo_rs,
    s2_ss, s2_rs, fo_ss, fo_rs,
):
    z = sizes
    DP, MP = z["DP"], z["MP"]
    NTOK, BT, CAP, ST, LR = z["NTOK"], z["BT"], z["CAP"], z["ST"], z["LR"]
    D, MH, RANK, KV, NB = z["D"], z["MH"], z["RANK"], z["KV"], z["NB"]
    SH, HC, Q, R, UN, RU, RD, RG, KC = (z[k] for k in ("SH", "HC", "Q", "R", "UN", "RU", "RD", "RG", "KC"))
    KH = KV // 2
    NK = MH // KC
    QB = Q // R
    OWN = DP * MP
    c = lax.axis_index("grp")
    e = lax.axis_index("dp")
    m = lax.axis_index("mp")
    p, u = e % 2, e // 2
    oc = 1 - c
    t0 = (p + m // 2 + c) % 2
    owner = e * MP + m
    pending = []

    def copy(src, dst, ssem, rsem, dp=None, mp=None, grp=None):
        device = {"grp": c if grp is None else grp, "dp": e if dp is None else dp, "mp": m if mp is None else mp}
        return pltpu.make_async_remote_copy(
            src_ref=src, dst_ref=dst, send_sem=ssem, recv_sem=rsem, device_id=device, device_id_type=MESH
        )

    def send(*args, **kw):
        made = copy(*args, **kw)
        made.start()
        pending.append(made)

    def landed(dst, ssem, rsem):
        copy(dst, dst, ssem, rsem, grp=oc).wait_recv()

    barrier = pltpu.get_barrier_semaphore()
    devices = 2 * OWN
    place = (c * DP + e) * MP + m

    def greet(i, carry):
        other = (place + i) % devices
        device = {"grp": other // OWN, "dp": other // MP % DP, "mp": other % MP}
        pl.semaphore_signal(barrier, inc=1, device_id=device, device_id_type=MESH)
        return carry

    lax.fori_loop(1, devices, greet, 0)

    half = c * HC
    loads = []
    for k in range(NK):
        one = pltpu.make_async_copy(
            enc_weight.at[pl.ds(k * KC, KC), pl.ds(half, HC)], ebuf.at[pl.ds(k * KC, KC), :], e_sem.at[k]
        )
        loads.append(one)
    text_load = pltpu.make_async_copy(text_rows, txt, t_sem)
    own_load = pltpu.make_async_copy(hidden, hid.at[pl.ds(m * NTOK, NTOK), :], own_sem)
    own_load.start()
    text_load.start()
    for one in loads:
        one.start()

    RH = RANK // 2
    low_half = c * RH
    at[e, m, pl.ds(low_half, RH), :] = llm_frozen[pl.ds(pl.multiple_of(low_half, 16), RH), :]
    for packed, row in ((gain_in, gain_ref), (enc_bias_in, enc_bias), (bias_in, bias_ref)):
        wide = packed[...].astype(F32)
        for i in range(wide.shape[0]):
            row[:, i * 128 : (i + 1) * 128] = wide[i : i + 1]
    rows = CAP * DP
    order_i = lax.broadcasted_iota(jnp.int32, (rows, rows), 0)
    order_j = lax.broadcasted_iota(jnp.int32, (rows, rows), 1)
    order = (order_j == order_i % CAP * DP + order_i // CAP).astype(BF16)
    sorted_targets = dot(order, targets[pl.ds(0, rows), pl.ds(c * KH, KH)]).astype(BF16)
    length = seq_length[...].astype(F32)
    for i in range(DP):
        for j in range(MP):
            block = sorted_targets[i * CAP : (i + 1) * CAP, j * NB : (j + 1) * NB]
            tail = jnp.broadcast_to(length, (ST - CAP, NB)).astype(BF16)
            tgs[i, j] = jnp.concatenate([block, tail], axis=0)

    pl.semaphore_wait(barrier, devices - 1)

    w_sends = []

    def send_weights():
        w_row = owner * R
        w_m = w_row // SH
        w_t = w_row % SH // Q
        w_slot = w_row % Q // R
        w_core = w_t // 2
        w_par = (w_t % 2 + w_t // 2 + w_m // 2) % 2
        for i in range((UN + 1) // 2):
            w_u = 2 * i + c
            there = 2 * w_u + w_par
            self_case = (there == e) & (w_m == m) & (w_core == c)
            live = w_u < UN
            away = copy(value_weight, wq.at[w_slot], w_ss.at[i], w_rs.at[w_slot], dp=there, mp=w_m, grp=w_core)
            near = pltpu.make_async_copy(value_weight, wq.at[w_slot], w_rs.at[w_slot])
            w_sends.append((live & jnp.logical_not(self_case), away))

            @pl.when(live & jnp.logical_not(self_case))
            def _():
                away.start()

            @pl.when(live & self_case)
            def _():
                near.start()

    for i in range(1, DP):
        mine = at.at[e, m, pl.ds(low_half, RH), :]
        send(mine, mine, a1_ss.at[i], a1_rs.at[i], dp=(e + i) % DP)
    NH = NTOK // 2
    hid_rows = pl.ds(m * NTOK + c * NH, NH)
    for k in range(NK):
        cols = pl.ds(k * KC, KC)
        for i in range(1, MP):
            send(hidden.at[pl.ds(c * NH, NH), cols], hid.at[hid_rows, cols], h_ss.at[k, i], h_rs.at[k, i], mp=(m + i) % MP)
    tgr[e, m] = tgs[e, m]

    def norm_text():
        text_load.wait()
        TR = 16
        CW = min(D, 1024)

        def text_norm(i, carry):
            r = pl.ds(i * TR, TR)
            total = jnp.zeros((TR, 128), F32)
            for k in range(D // CW):
                part = txt[r, pl.ds(k * CW, CW)].astype(F32)
                part = part * part
                for n in range(CW // 128):
                    total = total + part[:, n * 128 : (n + 1) * 128]
            inverse = lax.rsqrt(jnp.sum(total, axis=1, keepdims=True) / D + epsilon)
            for k in range(D // CW):
                cols = pl.ds(k * CW, CW)
                txt[r, cols] = (txt[r, cols].astype(F32) * inverse * gain_ref[:, cols]).astype(BF16)
            return carry

        lax.fori_loop(0, LR // TR, text_norm, 0)

    if NORM_AT == 0:
        norm_text()

    for i in range(1, DP):
        there = at.at[(e + DP - i) % DP, m, pl.ds(low_half, RH), :]
        landed(there, a1_ss.at[i], a1_rs.at[i])
    if W_AT == 0:
        send_weights()
    for i in range(1, MP):
        mine = at.at[:, m, pl.ds(low_half, RH), :]
        send(mine, mine, a2_ss.at[i], a2_rs.at[i], mp=(m + i) % MP)

    if W_AT == 1:
        send_weights()

    if NORM_AT == 1:
        norm_text()

    own_load.wait()
    TN = min(HC, 256)
    for k in range(NK):
        cols = pl.ds(k * KC, KC)
        for i in range(1, MP):
            peer = (m + MP - i) % MP
            there = hid.at[pl.ds(peer * NTOK + c * NH, NH), cols]
            landed(there, h_ss.at[k, i], h_rs.at[k, i])
            send(there, there, hf_ss.at[k, i], hf_rs.at[k, i], grp=oc)
        loads[k].wait()
        for i in range(1, MP):
            peer = (m + MP - i) % MP
            there = hid.at[pl.ds(peer * NTOK + oc * NH, NH), cols]
            landed(there, hf_ss.at[k, i], hf_rs.at[k, i])

        def product(n, carry):
            part = dot(hid[:, cols], ebuf[cols, pl.ds(n * TN, TN)])
            if k == 0:
                acc[:, pl.ds(n * TN, TN)] = part
            else:
                acc[:, pl.ds(n * TN, TN)] += part
            return carry

        lax.fori_loop(0, HC // TN, product, 0)
        low_part = dot(hid[:, cols], enc_frozen[:, cols], NT)
        if k == 0:
            acc_low[...] = low_part
        else:
            acc_low[...] += low_part
    enc_low = acc_low[...].astype(BF16)
    enc_low_t = dot(eye(RANK), enc_low, NT)
    squares = jnp.zeros((BT, 128), F32)
    for n in range(HC // TN):
        cols = pl.ds(n * TN, TN)
        shifted = pl.ds(half + n * TN, TN)
        merged = acc[:, cols] + enc_bias[:, shifted] + dot(enc_low, enc_adapter[:, shifted])
        merged = merged.astype(BF16)
        img[:, cols] = merged
        wide = merged.astype(F32)
        square = wide * wide
        for i in range(TN // 128):
            squares = squares + square[:, i * 128 : (i + 1) * 128]
        scaled = (wide * gain_ref[:, pl.ds(m * SH + half + n * TN, TN)]).astype(BF16)
        xq[n * TN // Q, :, n * TN % Q : n * TN % Q + TN] = scaled
    pair = e + 1 - 2 * p
    send(xq.at[1 - t0], xr, x_ss, x_rs, dp=pair)
    if TG_AT == 0:
        for i in range(1, OWN):
            other = (owner + i) % OWN
            od, om = other // MP, other % MP
            send(tgs.at[od, om], tgr.at[e, m], tg_ss.at[i], tg_rs.at[i], dp=od, mp=om)

    for i in range(1, MP):
        there = at.at[:, (m + MP - i) % MP, pl.ds(low_half, RH), :]
        landed(there, a2_ss.at[i], a2_rs.at[i])
    mine = at.at[:, :, pl.ds(low_half, RH), :]
    send(mine, mine, a3_ss, a3_rs, grp=oc)
    landed(at.at[:, :, pl.ds(oc * RH, RH), :], a3_ss, a3_rs)

    first = (m * SH + half) // R
    low_part = jnp.zeros((RANK, BT), F32)
    for i in range(HC // R):
        q = first + i
        x = xq[i * R // Q, :, i * R % Q : i * R % Q + R]
        low_part = low_part + dot(at[q // MP, q % MP], x, NT)
    total = jnp.broadcast_to(jnp.sum(squares, axis=1, keepdims=True), (BT, 128))
    los[...] = jnp.concatenate([low_part, total.T[:8]], axis=0)
    me8 = m * 2 + c
    send(los, lop, lp_ss, lp_rs, grp=oc)
    landed(lop, lp_ss, lp_rs)
    lor[m] = los[...] + lop[...]
    for i in range(1, MP):
        send(lor.at[m], lor.at[m], lo_ss.at[i], lo_rs.at[i], mp=(m + i) % MP)
    if TG_AT == 1:
        for i in range(1, OWN):
            other = (owner + i) % OWN
            od, om = other // MP, other % MP
            send(tgs.at[od, om], tgr.at[e, m], tg_ss.at[i], tg_rs.at[i], dp=od, mp=om)

    def text_low(q, carry):
        part = txt[:, pl.ds(pl.multiple_of(q * R, 128), R)]
        return carry + dot(part, at[q // MP, q % MP], NT)

    text_low_n = lax.fori_loop(0, OWN, text_low, jnp.zeros((LR, RANK), F32))
    text_low_b = text_low_n.astype(BF16)
    text_low_t = jnp.concatenate([text_low_b.astype(F32), jnp.zeros((LR, 128 - RANK), F32)], axis=1).T[:RANK]
    place_row = lax.broadcasted_iota(jnp.int32, (8, LR), 1)
    count = jnp.zeros((8, LR), F32)
    for i in range(DP):
        named = (dest[:, i * BT : (i + 1) * BT] == owner).astype(F32)
        named = jnp.sum(named, axis=1, keepdims=True)
        count = jnp.where(place_row % DP == i, jnp.broadcast_to(named, (8, LR)), count)
    replaced = (place_row < CAP * DP) & ((place_row // DP).astype(F32) < count)
    live = (place_row.astype(F32) < jnp.broadcast_to(length, (8, LR))) & jnp.logical_not(replaced)
    live = jnp.where(live, 1.0, 0.0)[:1]
    text_low_m = (text_low_t * live).astype(BF16)
    scale = 1.0 / length
    here8 = p * MP + m
    for j in range(MP):
        for i in range(2):
            col = pl.multiple_of(j * SH + half + i * Q, 128)
            gs[j, i] = (dot(text_low_m, txt[:, pl.ds(col, Q)]) * scale).astype(BF16)
    for i in range(1, 2 * MP):
        other = (here8 + i) % (2 * MP)
        gp, gm = other // MP, other % MP
        send(gs.at[gm, (gp + gm // 2 + c) % 2], gr.at[p, m], g_ss.at[i], g_rs.at[i], dp=2 * u + gp, mp=gm)
    gr[p, m] = gs[m, t0]
    text_y = dot(text_low_b, adapter_ref[:, pl.ds(c * KH, KH)])
    text_y = text_y + bias_ref[:, pl.ds(c * KH, KH)] - targets[:, pl.ds(c * KH, KH)].astype(F32)
    high = text_y.astype(BF16)
    rest = (text_y - high.astype(F32)).astype(BF16)
    text_grad = (dot(text_low_m, high) + dot(text_low_m, rest)) * scale

    if TG_AT == 2:
        for i in range(1, OWN):
            other = (owner + i) % OWN
            od, om = other // MP, other % MP
            send(tgs.at[od, om], tgr.at[e, m], tg_ss.at[i], tg_rs.at[i], dp=od, mp=om)

    for i in range(QB):
        landed(wq.at[i], w_ss.at[0], w_rs.at[i])

    def values_of(x, where, first_col):
        for n in range(KH // TN):
            cols = pl.ds(pl.multiple_of(first_col + n * TN, 128), TN)
            part = dot(x[:, :R], wq[0, :, cols])
            for i in range(1, QB):
                part = part + dot(x[:, i * R : (i + 1) * R], wq[i, :, cols])
            where[:, n * TN : (n + 1) * TN] = part.astype(where.dtype)

    values_of(xq[t0], vps.at[p], oc * KH)
    send(vps.at[p], vpr.at[p], vp_ss.at[0], vp_rs.at[0], grp=oc)
    landed(xr, x_ss, x_rs)
    values_of(xr[...], vps.at[1 - p], oc * KH)
    send(vps.at[1 - p], vpr.at[1 - p], vp_ss.at[1], vp_rs.at[1], grp=oc)
    values_of(xq[t0], vown.at[p], c * KH)
    values_of(xr[...], vown.at[1 - p], c * KH)
    landed(vpr.at[p], vp_ss.at[0], vp_rs.at[0])
    landed(vpr.at[1 - p], vp_ss.at[1], vp_rs.at[1])
    for i in range(2):
        both = (vown[i] + vpr[i]).astype(BF16)
        for j in range(MP):
            vs[i, j] = both[:, j * NB : (j + 1) * NB]
    for i in range(1, 2 * MP):
        other = (here8 + i) % (2 * MP)
        gp, gm = other // MP, other % MP
        send(vs.at[gp, gm], vr.at[p, m], v_ss.at[i], v_rs.at[i], dp=2 * u + gp, mp=gm)
    vr[p, m] = vs[p, m]

    for i in range(1, OWN):
        other = (owner + OWN - i) % OWN
        landed(tgr.at[other // MP, other % MP], tg_ss.at[i], tg_rs.at[i])
    block_dest = dest[:, pl.ds(pl.multiple_of(e * BT, 128), BT)].astype(F32)
    block_dest = jnp.broadcast_to(block_dest, (128, BT)).T
    marks = block_dest == lax.broadcasted_iota(jnp.int32, (BT, 128), 1).astype(F32)
    before = lax.broadcasted_iota(jnp.int32, (BT, BT), 0) > lax.broadcasted_iota(jnp.int32, (BT, BT), 1)
    counted = dot(before.astype(BF16), marks.astype(BF16))
    slot = jnp.sum(jnp.where(marks, counted, 0.0), axis=1, keepdims=True)
    base = block_dest[:, :1] * ST
    table_rows = lax.broadcasted_iota(jnp.int32, (BT, OWN * ST), 1).astype(F32)
    table = tgr[...].reshape(OWN * ST, NB)
    image_targets = dot((table_rows == base + slot).astype(BF16), table)
    image_length = dot((table_rows == base + CAP).astype(BF16), table)
    position = slot * DP + e.astype(F32)
    weight = jnp.where(position < image_length, 1.0 / image_length, 0.0)

    gathered = jnp.zeros((RANK + 8, BT), F32)
    for i in range(1, MP):
        landed(lor.at[(m + MP - i) % MP], lo_ss.at[i], lo_rs.at[i])
    for i in range(MP):
        gathered = gathered + lor[i]
    inverse_row = lax.rsqrt(gathered[RANK : RANK + 1] / D + epsilon)
    low_t = (gathered[:RANK] * inverse_row).astype(BF16)
    turned = jnp.concatenate(
        [low_t.astype(F32), jnp.broadcast_to(inverse_row, (128 - RANK, BT))], axis=0
    ).T
    low = turned[:, :RANK].astype(BF16)
    inverse = turned[:, RANK : RANK + 1]

    for i in range(1, 2 * MP):
        other = (here8 + 2 * MP - i) % (2 * MP)
        landed(vr.at[other // MP, other % MP], v_ss.at[i], v_rs.at[i])
    product_sum = jnp.zeros((BT, NB), F32)
    for i in range(2):
        for j in range(MP):
            product_sum = product_sum + vr[i, j].astype(F32)
    own_cols = pl.ds(pl.multiple_of(c * KH + m * NB, 128), NB)
    plain = product_sum * inverse + dot(low, adapter_ref[:, own_cols])
    dv = plain + bias_ref[:, own_cols] - image_targets
    dv = (dv * weight).astype(BF16)
    along = jnp.sum(dv.astype(F32) * plain, axis=1, keepdims=True)
    ss[...] = jnp.broadcast_to(along, (BT, 128)).T[:8]
    for i in range(1, 2 * MP):
        other = (me8 + i) % (2 * MP)
        send(ss, sr.at[me8], s_ss.at[i], s_rs.at[i], mp=other // 2, grp=other % 2)
    sr[me8] = ss[...]
    h_part = joined(dot(split(enc_low_t * inverse_row), dv))
    y_part = dot(low_t, dv)
    for i in range(DP):
        hys[i, 0] = h_part[i * RD : (i + 1) * RD]
        hys[i, 1] = y_part[i * RD : (i + 1) * RD]
    for i in range(1, DP):
        there = (e + i) % DP
        send(hys.at[there], hyr.at[e], hy_ss.at[i], hy_rs.at[i], dp=there)
    hyr[e] = hys[e]

    for i in range(1, 2 * MP):
        other = (here8 + 2 * MP - i) % (2 * MP)
        landed(gr.at[other // MP, other % MP], g_ss.at[i], g_rs.at[i])
    g_sum = jnp.zeros((RANK, Q), F32)
    for i in range(2):
        for j in range(MP):
            g_sum = g_sum + gr[i, j].astype(F32)
    g_pair = split(g_sum)

    def through(cols):
        part = dot(g_pair[:, :R], wq[0, :, cols])
        for i in range(1, QB):
            part = part + dot(g_pair[:, i * R : (i + 1) * R], wq[i, :, cols])
        return joined(part)

    ys[...] = through(pl.ds(oc * KH, KH))
    send(ys, yr, yp_ss, yp_rs, grp=oc)
    text_grad = text_grad + through(pl.ds(c * KH, KH))
    landed(yr, yp_ss, yp_rs)
    text_grad = text_grad + yr[...]
    for i in range(DP):
        for j in range(MP):
            yrs[i, j] = text_grad[i * RD : (i + 1) * RD, j * NB : (j + 1) * NB]
    for i in range(1, OWN):
        other = (owner + i) % OWN
        od, om = other // MP, other % MP
        send(yrs.at[od, om], yrr.at[e, m], yr_ss.at[i], yr_rs.at[i], dp=od, mp=om)
    yrr[e, m] = yrs[e, m]

    for i in range(1, 2 * MP):
        other = (me8 + 2 * MP - i) % (2 * MP)
        landed(sr.at[other], s_ss.at[i], s_rs.at[i])
    along_row = jnp.zeros((8, BT), F32)
    for i in range(2 * MP):
        along_row = along_row + sr[i]
    factor = along_row[:1] * inverse_row * inverse_row / D
    second_pair = split(enc_low_t * factor)
    for i in range(2):
        second = joined(dot(second_pair, img[:, pl.ds(i * Q, Q)])).astype(BF16)
        for j in range(UN):
            s2s[i, j] = second[j * RU : (j + 1) * RU]
    for i in range(1, DP):
        there = (e + i) % DP
        send(s2s.at[(there % 2 + c + m // 2) % 2, there // 2], s2r.at[e], s2_ss.at[i], s2_rs.at[i], dp=there)
    s2r[e] = s2s[t0, u]

    for i in range(1, DP):
        landed(hyr.at[(e + DP - i) % DP], hy_ss.at[i], hy_rs.at[i])
    hy = hyr[0]
    for i in range(1, DP):
        hy = hy + hyr[i]
    hbs[...] = hy[0]
    unit = (p * 2 + c) * MP + m
    for i in range(1, 4 * MP):
        other = (unit + i) % (4 * MP)
        send(
            hbs, hb.at[p, c, m], hb_ss.at[i], hb_rs.at[i],
            dp=2 * u + other // (2 * MP), grp=other // MP % 2, mp=other % MP,
        )
    hb[p, c, m] = hbs[...]
    for i in range(1, OWN):
        other = (owner + OWN - i) % OWN
        landed(yrr.at[other // MP, other % MP], yr_ss.at[i], yr_rs.at[i])
    y_sum = hy[1]
    for i in range(DP):
        for j in range(MP):
            y_sum = y_sum + yrr[i, j]
    yos[...] = y_sum
    DH = DP // 2
    y_core = e // DH
    y_row = e % DH
    y_there = out_llm.at[y_row, :, own_cols]
    for i in range(1, OWN):
        other = (owner + i) % OWN
        send(yos, y_there, yo_ss.at[i], yo_rs.at[y_row, m, c], dp=other // MP, mp=other % MP, grp=y_core)
    y_away = copy(yos, y_there, yo_ss.at[0], yo_rs.at[y_row, m, c], grp=oc)

    @pl.when(y_core == c)
    def _():
        out_llm[y_row, :, own_cols] = yos[...]

    @pl.when(y_core != c)
    def _():
        y_away.start()

    for i in range(1, 4 * MP):
        other = (unit + 4 * MP - i) % (4 * MP)
        landed(hb.at[other // (2 * MP), other // MP % 2, other % MP], hb_ss.at[i], hb_rs.at[i])
    h_all = jnp.concatenate(
        [
            jnp.concatenate([hb[i, j, k] for j in range(2) for k in range(MP)], axis=1)
            for i in range(2)
        ],
        axis=0,
    )
    h_pair = split(h_all)
    h_low = split(joined(dot(h_pair, adapter_ref[...], NT)))
    quarter = m * SH + half + t0 * Q
    parts = []
    for i in range(QB):
        q = quarter // R + i
        part = joined(dot(h_pair, wq[i], NT)) + joined(dot(h_low, at[q // MP, q % MP]))
        parts.append(part * gain_ref[:, pl.ds(pl.multiple_of(quarter + i * R, 128), R)])
    result = jnp.concatenate(parts, axis=1)
    for i in range(1, DP):
        landed(s2r.at[(e + DP - i) % DP], s2_ss.at[i], s2_rs.at[i])
    for i in range(DP):
        result = result - s2r[i].astype(F32)
    fo[...] = result
    UH = UN // 2
    f_core = u // UH
    f_unit = u % UH
    f_there = fin.at[f_unit, p, c]
    for i in range(1, DP):
        send(fo, f_there, fo_ss.at[i], fo_rs.at[f_unit, p, c], dp=(e + i) % DP, grp=f_core)
    f_away = copy(fo, f_there, fo_ss.at[0], fo_rs.at[f_unit, p, c], grp=oc)

    @pl.when(f_core == c)
    def _():
        fin[f_unit, p, c] = fo[...]

    @pl.when(f_core != c)
    def _():
        f_away.start()

    for i in range(DH):
        for j in range(MP):
            for k in range(2):
                other = copy(yos, out_llm.at[i, :, pl.ds(k * KH + j * NB, NB)], yo_ss.at[0], yo_rs.at[i, j, k], grp=oc)

                @pl.when(jnp.logical_not((y_core == c) & (y_row == i) & (m == j) & (c == k)))
                def _():
                    other.wait_recv()

    for i in range(UH):
        for j in range(2):
            for k in range(2):
                t_other = (j + m // 2 + k) % 2
                cols = pl.ds(pl.multiple_of(k * HC + t_other * Q, 128), Q)
                arrival = copy(fo, fin.at[i, j, k], fo_ss.at[0], fo_rs.at[i, j, k], grp=oc)

                @pl.when(jnp.logical_not((f_core == c) & (f_unit == i) & (p == j) & (c == k)))
                def _():
                    arrival.wait_recv()

                out_enc[pl.ds(i * RU, RU), cols] = fin[i, j, k].astype(F32)

    for one in pending:
        one.wait_send()
    for started, one in w_sends:

        @pl.when(started)
        def _():
            one.wait_send()

    @pl.when(y_core != c)
    def _():
        y_away.wait_send()

    @pl.when(f_core != c)
    def _():
        f_away.wait_send()


def body(
    hidden, enc_weight, enc_bias, enc_frozen, enc_adapter, text_rows, norm_gain, value_weight,
    value_bias, llm_frozen, llm_adapter, targets, dest_owner, seq_length,
):
    DP, MP = lax.axis_size("dp"), lax.axis_size("mp")
    OWN = DP * MP
    NTOK, MH = hidden.shape
    BT = NTOK * MP
    LR, D = text_rows.shape
    RANK = enc_frozen.shape[1]
    KV = llm_adapter.shape[1]
    CAP = 2 * BT // OWN
    ST = CAP + 8
    ST = ST + -ST % 16
    SH = enc_weight.shape[1]
    HC, Q = SH // 2, SH // 4
    R = value_weight.shape[0]
    UN = DP // 2
    RU, RD, RG = RANK // UN, RANK // DP, RANK // 2
    KH, NB = KV // 2, KV // (2 * MP)
    KC = 1024 if MH % 1024 == 0 else MH
    NK = MH // KC
    QB = Q // R
    RL = RANK + 8
    sizes = dict(
        DP=DP, MP=MP, NTOK=NTOK, BT=BT, CAP=CAP, ST=ST, LR=LR, D=D, MH=MH, RANK=RANK, KV=KV, NB=NB,
        SH=SH, HC=HC, Q=Q, R=R, UN=UN, RU=RU, RD=RD, RG=RG, KC=KC,
    )
    vmem = pl.BlockSpec(memory_space=pltpu.VMEM)
    hbm = pl.BlockSpec(memory_space=pl.ANY)
    V = pltpu.VMEM
    S = pltpu.SemaphoreType.DMA
    scratch = [
        V((1, D), F32), V((1, SH), F32), V((1, KV), F32),
        V((MH, HC), BF16), V((BT, MH), BF16), V((BT, HC), F32), V((BT, RANK), F32), V((BT, HC), BF16),
        V((2, BT, Q), BF16), V((BT, Q), BF16), V((QB, R, KV), BF16), V((DP, MP, RANK, R), BF16), V((LR, D), BF16),
        V((MP, 2, RANK, Q), BF16), V((2, MP, RANK, Q), BF16), V((DP, MP, ST, NB), BF16), V((DP, MP, ST, NB), BF16),
        V((RL, BT), F32), V((MP, RL, BT), F32),
        V((2, BT, KH), F32), V((2, BT, KH), F32), V((2, BT, KH), F32),
        V((2, MP, BT, NB), BF16), V((2, MP, BT, NB), BF16),
        V((RL, BT), F32),
        V((RANK, KH), F32), V((RANK, KH), F32), V((DP, MP, RD, NB), F32), V((DP, MP, RD, NB), F32),
        V((8, BT), F32), V((2 * MP, 8, BT), F32), V((DP, 2, RD, NB), F32), V((DP, 2, RD, NB), F32),
        V((RD, NB), F32), V((2, 2, MP, RD, NB), F32), V((RD, NB), F32),
        V((2, UN, RU, Q), BF16), V((DP, RU, Q), BF16), V((RU, Q), F32), V((UN // 2, 2, 2, RU, Q), F32),
        S((NK,)), S(()), S(()), S((NK, MP)), S((NK, MP)), S((NK, MP)), S((NK, MP)),
        S(((UN + 1) // 2,)), S((QB,)), S(()), S(()), S((DP,)), S((DP,)), S((MP,)), S((MP,)),
        S(()), S(()), S((OWN,)), S((OWN,)), S(()), S(()), S((2 * MP,)), S((2 * MP,)), S((2 * MP,)), S((2 * MP,)),
        S((2,)), S((2,)), S((2 * MP,)), S((2 * MP,)),
        S(()), S(()), S((OWN,)), S((OWN,)), S((2 * MP,)), S((2 * MP,)), S((DP,)), S((DP,)),
        S((4 * MP,)), S((4 * MP,)), S((OWN,)), S((DP // 2, MP, 2)),
        S((DP,)), S((DP,)), S((DP,)), S((UN // 2, 2, 2)),
    ]
    grad_enc, grad_llm = pl.pallas_call(
        functools.partial(kernel, sizes),
        out_shape=(
            jax.ShapeDtypeStruct((RG, SH), F32),
            jax.ShapeDtypeStruct((DP // 2, RD, KV), F32),
        ),
        in_specs=[hbm, hbm, vmem, vmem, vmem, hbm, vmem, hbm, vmem, vmem, vmem, vmem, vmem, vmem],
        out_specs=(vmem, vmem),
        scratch_shapes=scratch,
        compiler_params=pltpu.CompilerParams(
            collective_id=0, has_side_effects=True, vmem_limit_bytes=60 * 1024 * 1024
        ),
    )(
        hidden, enc_weight, enc_bias.reshape(-1, 128), enc_frozen.T, enc_adapter, text_rows,
        norm_gain.reshape(-1, 128), value_weight, value_bias.reshape(-1, 128), llm_frozen.T, llm_adapter,
        targets, dest_owner.T, seq_length.reshape(1, 1),
    )
    return grad_enc, grad_llm.reshape(RG, KV)


def solution(mesh):
    return jax.shard_map(
        body,
        mesh=mesh,
        in_specs=(
            P(("dp", "mp"), None), P(None, "mp"), P("mp"), P(), P(None, "mp"), P(("dp", "mp"), None), P(),
            P(("dp", "mp"), None), P(), P(("dp", "mp"), None), P(), P(("dp", "mp"), None), P(), P(("dp", "mp")),
        ),
        out_specs=(P("grp", "mp"), P("grp", None)),
        check_vma=False,
    )
```
